8 devices in a mesh: dp: 1 (over z), sw: 2 (over y), sh: 4 (over x, core).
Axes of the slice: x: 2, y: 2, z: 1, core: 2. Of those that a mesh axis runs over, the one named last changes fastest.
Arguments:
- act_in: bfloat16 [32, 48, 64, 40], P('dp', 'sh', 'sw')
- drop_mask: float32 [32, 2], P('dp')
- grad_out: bfloat16 [32, 48, 64, 40], P('dp', 'sh', 'sw')
- conv_w: bfloat16 [2, 7, 7, 40], replicated
- conv_b: float32 [2, 40], replicated
- norm_g: float32 [2, 40], replicated
- norm_b: float32 [2, 40], replicated
- fc1_w: bfloat16 [2, 40, 160], replicated
- fc1_b: float32 [2, 160], replicated
- grn_gamma: float32 [2, 160], replicated
- grn_beta: float32 [2, 160], replicated
- fc2_w: bfloat16 [2, 160, 40], replicated
- fc2_b: float32 [2, 40], replicated
Outputs:
- output 1: bfloat16 [32, 48, 64, 40], P('dp', 'sh', 'sw')
- output 2: bfloat16 [32, 48, 64, 40], P('dp', 'sh', 'sw')
- output 3: float32 [2, 7, 7, 40], P('dp')
- output 4: float32 [2, 40], P('dp')
- output 5: float32 [2, 40], P('dp')
- output 6: float32 [2, 40], P('dp')
- output 7: float32 [2, 40, 160], P('dp')
- output 8: float32 [2, 160], P('dp')
- output 9: float32 [2, 160], P('dp')
- output 10: float32 [2, 160], P('dp')
- output 11: float32 [2, 160, 40], P('dp')
- output 12: float32 [2, 40], P('dp')
All inputs are finite; a program needn't handle non-finite values.
Results may differ from the reference program's by a relative error of at most 0.0166898.
Values are sent between devices in bfloat16 or wider.
A program may use at most 1 GiB of HBM per device.

```python
import jax
import jax.numpy as jnp
from jax import lax

BATCH = 32
GRID_H = 4
GRID_W = 2
TILE_H = 12
TILE_W = 32
CHANNELS = 40

HEIGHT = TILE_H * GRID_H
WIDTH = TILE_W * GRID_W
HIDDEN = 4 * CHANNELS
N_DROP = max(1, BATCH // 4)
KEEP_SCALE = 4.0 / 3.0
EPSILON = 1e-6


def setup_inputs(seed: int = 0, part: int = 0) -> dict:
    root_key = jax.random.key(seed)
    shared = jax.random.split(root_key, 10)
    part_keys = jax.random.split(jax.random.fold_in(root_key, part), 6)
    img_shape = (BATCH, HEIGHT, WIDTH, CHANNELS)
    tile_shape = (BATCH, GRID_H, GRID_W, CHANNELS)

    def spread(tile_vals):
        return jnp.repeat(jnp.repeat(tile_vals, TILE_H, axis=1), TILE_W, axis=2)

    def normal(index, shape):
        return jax.random.normal(shared[index], shape, jnp.float32)

    images = jax.random.normal(part_keys[0], img_shape, jnp.float32) + 1.5 * spread(jax.random.normal(part_keys[1], tile_shape, jnp.float32))
    cotangent = (jax.random.normal(part_keys[2], img_shape, jnp.float32)
                 + 0.8 * spread(jax.random.normal(part_keys[3], tile_shape, jnp.float32))
                 + 0.6 * jax.random.normal(part_keys[4], (BATCH, 1, 1, CHANNELS), jnp.float32))
    mask_keys = jax.random.split(part_keys[5], 2)
    drop_rank = jnp.stack([jax.random.permutation(mask_keys[0], BATCH), jax.random.permutation(mask_keys[1], BATCH)], axis=1)
    drop_mask = jnp.where(drop_rank < N_DROP, 0.0, KEEP_SCALE).astype(jnp.float32)
    return dict(
        act_in=images.astype(jnp.bfloat16),
        drop_mask=drop_mask,
        grad_out=cotangent.astype(jnp.bfloat16),
        conv_w=(normal(0, (2, 7, 7, CHANNELS)) / 7.0).astype(jnp.bfloat16),
        conv_b=0.5 * normal(1, (2, CHANNELS)),
        norm_g=1.0 + 0.3 * normal(2, (2, CHANNELS)),
        norm_b=0.3 * normal(3, (2, CHANNELS)),
        fc1_w=(normal(4, (2, CHANNELS, HIDDEN)) * CHANNELS ** -0.5).astype(jnp.bfloat16),
        fc1_b=0.5 * normal(5, (2, HIDDEN)),
        grn_gamma=normal(6, (2, HIDDEN)),
        grn_beta=0.5 * normal(7, (2, HIDDEN)),
        fc2_w=(normal(8, (2, HIDDEN, CHANNELS)) * HIDDEN ** -0.5).astype(jnp.bfloat16),
        fc2_b=0.5 * normal(9, (2, CHANNELS)),
    )


def convnext_block(x_img, mask_val, weights):
    conv_w, conv_b, norm_g, norm_b, fc1_w, fc1_b, grn_gamma, grn_beta, fc2_w, fc2_b = weights
    x_float = x_img.astype(jnp.float32)
    conv_out = lax.conv_general_dilated(x_float[None], conv_w[:, :, None, :], (1, 1), ((3, 3), (3, 3)),
                                        dimension_numbers=('NHWC', 'HWIO', 'NHWC'),
                                        feature_group_count=CHANNELS)[0]
    conv_out = (conv_out + conv_b).astype(jnp.bfloat16).astype(jnp.float32)
    centered = conv_out - jnp.mean(conv_out, axis=-1, keepdims=True)
    normed = centered * lax.rsqrt(jnp.mean(centered * centered, axis=-1, keepdims=True) + EPSILON)
    n_act = (normed * norm_g + norm_b).astype(jnp.bfloat16).astype(jnp.float32)
    hidden = (jnp.einsum('hwc,ck->hwk', n_act, fc1_w) + fc1_b).astype(jnp.bfloat16).astype(jnp.float32)
    g_act = jax.nn.gelu(hidden, approximate=False)
    g_norm = jnp.sqrt(jnp.sum(g_act * g_act, axis=(0, 1)))
    grn_scale = g_norm / (jnp.mean(g_norm) + EPSILON)
    grn_out = (grn_gamma * (g_act * grn_scale) + grn_beta + g_act).astype(jnp.bfloat16).astype(jnp.float32)
    proj_out = jnp.einsum('hwk,kc->hwc', grn_out, fc2_w) + fc2_b
    return (x_float + mask_val * proj_out).astype(jnp.bfloat16)


def two_blocks(x_img, mask_row, weights):
    first_w = tuple(weight[0] for weight in weights)
    second_w = tuple(weight[1] for weight in weights)
    return convnext_block(convnext_block(x_img, mask_row[0], first_w), mask_row[1], second_w)


def reference(act_in, drop_mask, grad_out, conv_w, conv_b, norm_g, norm_b, fc1_w, fc1_b, grn_gamma, grn_beta, fc2_w, fc2_b):
    params = tuple(weight.astype(jnp.float32) for weight in (conv_w, conv_b, norm_g, norm_b, fc1_w, fc1_b, grn_gamma, grn_beta, fc2_w, fc2_b))

    def one_image(image_item):
        x_img, mask_row, d_img = image_item

        def forward(x_in, weights):
            return two_blocks(x_in, mask_row, weights)

        out_img, pullback = jax.vjp(forward, x_img, params)
        d_x, d_weights = pullback(d_img)
        return out_img, d_x, d_weights

    act_out, grad_in, weight_grads = lax.map(one_image, (act_in, drop_mask, grad_out))
    return (act_out, grad_in) + tuple(jnp.sum(per_image, axis=0) for per_image in weight_grads)
```

```python
import functools

import jax
import jax.numpy as jnp
import numpy as np
from jax import lax
from jax.experimental import pallas as pl
from jax.experimental.pallas import tpu as pltpu
from jax.sharding import PartitionSpec as P

EPS = 1e-6
F32 = jnp.float32
BF16 = jnp.bfloat16
MESH = pl.DeviceIdType.MESH
NG = 5
NPAIR = 24
ROWS = 224
KEEP = 4.0 / 3.0
FC1B, GAMMA, BETA, CONVB, NORMG, NORMB, FC2B = 0, 160, 320, 480, 520, 560, 600


LANE = 128
PXL = 256
PXP = 512
SUB = 8
CH = 40
HID = 160
IMG = 32
PR = 16
TQ = 96
CHP = 48
BAND = 1024
PIX = 384
HIDP = 176
CHQ = 88
HALFL = 64
PADH = 12
ZERO = 0.0
ONE = 1.0
TAP = 7
TILEH = 6
QUAD = 4
RAD = 3
PAIR = 2
I0 = 0
I1 = 1


def nt_dot(a, b):
    return lax.dot_general(a, b, (((I1,), (I1,)), ((), ())), preferred_element_type=F32)


def dot(a, b):
    return jnp.dot(a, b, preferred_element_type=F32)


def kernel(xin, gin, mask_in, taps, b_fc1, gamma, beta, b_conv, g_norm, b_norm, b_fc2, w1, w2t,
           y_out, dx_out, gr_out,
           xf, gout, mask, eb, cols, w1t, w2, x1, x2, dp, dbuf, nbuf, hbuf, drbuf, dmid, tbuf,
           acc_g2, acc_cross, acc_beta, acc_n, acc_f1, acc_f2, gvec, sbuf, gnbuf, qbuf,
           ru, rd, rc, sc, sa, ra, gb, grx, gs,
           hs_sem, hr_sem, as_sem, ar_sem, gs_sem, gr_sem, as2_sem, ar2_sem):
    sw = lax.axis_index('sw')
    sh = lax.axis_index('sh')
    me = sw * QUAD + sh
    other_w = I1 - sw

    def peer(d):
        f = lax.rem(me + d, SUB)
        return {'sw': f // QUAD, 'sh': lax.rem(f, QUAD)}

    barrier = pltpu.get_barrier_semaphore()
    for d in range(I1, SUB):
        pl.semaphore_signal(barrier, inc=I1, device_id=peer(d), device_id_type=MESH)
    pl.semaphore_wait(barrier, TAP)

    def setup():
        spots = ((b_fc1, FC1B), (gamma, GAMMA), (beta, BETA), (b_conv, CONVB),
                 (g_norm, NORMG), (b_norm, NORMB), (b_fc2, FC2B))
        for k in range(PAIR):
            for ref, at in spots:
                n = ref.shape[I1]
                row = jnp.broadcast_to(ref[k:k + I1, :], (LANE, n))
                cols[k, at:at + n, :] = jnp.transpose(row)
            m = jnp.concatenate([mask_in[k:k + I1, :]] * SUB, axis=I1)
            mask[k] = jnp.broadcast_to(m, (SUB, PXL))
            w1t[k] = jnp.transpose(jnp.concatenate([w1[k].astype(F32), jnp.zeros((SUB, HID), F32)], axis=I0)).astype(BF16)
            w2[k] = jnp.transpose(w2t[k].astype(F32)).astype(BF16)
        eb[...] = jnp.zeros_like(eb)
        place = lax.broadcasted_iota(jnp.int32, (PAIR, LANE), I1) // SUB

        def taps_row(i, carry):
            rows = [jnp.concatenate([taps[i, j].astype(F32), jnp.zeros((PAIR, CHQ), F32)], axis=I1) for j in range(TAP)]
            for g in range(NG):
                fwd = jnp.zeros((PAIR, LANE), F32)
                bwd = jnp.zeros((PAIR, LANE), F32)
                for j in range(TAP):
                    fwd = jnp.where(place == j, pltpu.roll(rows[j], (LANE + SUB * (j - g)) % LANE, I1), fwd)
                    bwd = jnp.where(place == TILEH - j, pltpu.roll(rows[j], (LANE + SUB * (TILEH - j - g)) % LANE, I1), bwd)
                eb[I0, g, i, I0:PAIR, :] = fwd
                eb[I1, g, TILEH - i, I0:PAIR, :] = bwd
            return carry
        lax.fori_loop(I0, TAP, taps_row, I0)

    def load_tiles(src, store):
        def widen(b, carry):
            xf[pl.ds(pl.multiple_of(b * PIX, PIX), PIX), :] = src[b].reshape(PIX, CH).astype(F32)
            return carry
        lax.fori_loop(I0, IMG, widen, I0)
        unit = jnp.where(lax.broadcasted_iota(jnp.int32, (CH, CH), I0) == lax.broadcasted_iota(jnp.int32, (CH, CH), I1),
                         ONE, ZERO).astype(BF16)

        def step(i, carry):
            first = (i // QUAD) * IMG + lax.rem(i, QUAD) * PAIR
            px = []
            for q in range(PAIR):
                rows = [xf[pl.ds(first + (q + hb * 192 + wb * SUB), IMG, stride=PIX), :]
                        for hb in range(PAIR) for wb in range(QUAD)]
                px.append(nt_dot(unit, jnp.concatenate(rows, axis=I0).astype(BF16)))
            for g in range(NG):
                store(g, i, jnp.concatenate([p[SUB * g:SUB * g + SUB] for p in px], axis=I0).astype(BF16))
            return carry
        lax.fori_loop(I0, NPAIR, step, I0)

    def col(k, off, n, width):
        piece = cols[k, off:off + n, :]
        return jnp.concatenate([piece] * (width // LANE), axis=I1)

    lane128 = lax.broadcasted_iota(jnp.int32, (SUB, LANE), I1)
    grp = lane128 // IMG

    def halo_copies(src, e):
        up = {'sw': sw, 'sh': jnp.maximum(sh - I1, I0)}
        down = {'sw': sw, 'sh': jnp.minimum(sh + I1, RAD)}
        upx = {'sw': other_w, 'sh': jnp.maximum(sh - I1, I0)}
        downx = {'sw': other_w, 'sh': jnp.minimum(sh + I1, RAD)}

        def cp(s, d, i, dev):
            return pltpu.make_async_remote_copy(
                src_ref=s, dst_ref=d, send_sem=hs_sem.at[e, i], recv_sem=hr_sem.at[e, i],
                device_id=dev, device_id_type=MESH)
        return (
            lambda: cp(src.at[:, TILEH:9, PAIR:TILEH, :, LANE:PXL], ru.at[e], I0, down),
            lambda: cp(src.at[:, RAD:TILEH, PAIR:TILEH, :, I0:LANE], rd.at[e], I1, up),
            lambda: cp(sc.at[e], rc.at[e, RAD:15], PAIR, {'sw': other_w, 'sh': sh}),
            lambda: cp(sc.at[e, 9:PADH], rc.at[e, I0:RAD], RAD, downx),
            lambda: cp(sc.at[e, I0:RAD], rc.at[e, 15:18], QUAD, upx),
        )

    def halo_start(src, e):
        copies = halo_copies(src, e)

        @pl.when(sh < RAD)
        def _():
            copies[I0]().start()

        @pl.when(sh > I0)
        def _():
            copies[I1]().start()
        first = QUAD - PAIR * sw

        def pack(h, carry):
            for half in range(PAIR):
                ls = slice(half * LANE, half * LANE + LANE)
                pieces = []
                for g in range(NG):
                    v = src[g, RAD + h, pl.ds(first, PAIR), :, ls].astype(F32).reshape(QUAD, SUB, LANE)
                    out = jnp.zeros((SUB, LANE), F32)
                    for q in range(QUAD):
                        shift = lax.rem(q * IMG + IMG * (I1 - sw), LANE)
                        out = jnp.where(grp == q, pltpu.roll(v[q], shift, I1), out)
                    pieces.append(out)
                sc[e, TILEH * half + h] = jnp.concatenate(pieces, axis=I0).astype(BF16)
            return carry
        lax.fori_loop(I0, TILEH, pack, I0)
        copies[PAIR]().start()

        @pl.when(sh < RAD)
        def _():
            copies[RAD]().start()

        @pl.when(sh > I0)
        def _():
            copies[QUAD]().start()

        @pl.when(sh == I0)
        def _():
            ru[e] = jnp.zeros(ru.shape[I1:], BF16)
            rc[e, I0:RAD] = jnp.zeros((RAD, CH, LANE), BF16)

        @pl.when(sh == RAD)
        def _():
            rd[e] = jnp.zeros(rd.shape[I1:], BF16)
            rc[e, 15:18] = jnp.zeros((RAD, CH, LANE), BF16)

    def halo_finish(src, e):
        copies = halo_copies(src, e)

        @pl.when(sh < RAD)
        def _():
            copies[I0]().wait_send()
            copies[RAD]().wait_send()
            copies[I1]().wait_recv()
            copies[QUAD]().wait_recv()

        @pl.when(sh > I0)
        def _():
            copies[I1]().wait_send()
            copies[QUAD]().wait_send()
            copies[I0]().wait_recv()
            copies[RAD]().wait_recv()
        copies[PAIR]().wait()
        for r in range(RAD):
            src[:, r, PAIR:TILEH, :, LANE:PXL] = src[:, TILEH + r, PAIR:TILEH, :, I0:LANE]
            src[:, r, PAIR:TILEH, :, I0:LANE] = ru[e, :, r]
            src[:, 9 + r, PAIR:TILEH, :, I0:LANE] = src[:, RAD + r, PAIR:TILEH, :, LANE:PXL]
            src[:, 9 + r, PAIR:TILEH, :, LANE:PXL] = rd[e, :, r]
        is_left = (lane128 < IMG)
        is_right = (lane128 >= TQ)
        keep_left = jnp.where(sw == I1, ONE, ZERO)
        keep_right = jnp.where(sw == I0, ONE, ZERO)

        def pad(h, carry):
            for half in range(PAIR):
                ls = slice(half * LANE, half * LANE + LANE)
                strip = rc[e, h + TILEH * half].astype(F32).reshape(NG, SUB, LANE)
                for g in range(NG):
                    hi = src[g, h, QUAD:TILEH, :, ls].astype(F32).reshape(QUAD, SUB, LANE)
                    lo = src[g, h, PAIR:QUAD, :, ls].astype(F32).reshape(QUAD, SUB, LANE)
                    left, right = [], []
                    for q in range(QUAD):
                        shift = lax.rem(jnp.where(sw == I1, LANE - q * IMG, 224 - q * IMG), LANE)
                        edge = pltpu.roll(strip[g], shift, I1)
                        left.append(jnp.where(is_left, edge * keep_left, pltpu.roll(hi[q], IMG, I1)))
                        right.append(jnp.where(is_right, edge * keep_right, pltpu.roll(lo[q], TQ, I1)))
                    src[g, h, I0:PAIR, :, ls] = jnp.concatenate(left, axis=I0).reshape(PAIR, PR, LANE).astype(BF16)
                    src[g, h, TILEH:SUB, :, ls] = jnp.concatenate(right, axis=I0).reshape(PAIR, PR, LANE).astype(BF16)
            return carry
        lax.fori_loop(I0, PADH, pad, I0)

    def fold(ref):
        v = ref[:, I0:LANE] + ref[:, LANE:PXL]
        v = v + pltpu.roll(v, IMG, I1)
        return v + pltpu.roll(v, HALFL, I1)

    def pack_sums(v):
        gq = lax.broadcasted_iota(jnp.int32, (CH, LANE), I1) // IMG
        out = v[I0:CH]
        for q in range(I1, QUAD):
            out = jnp.where(gq == q, v[CH * q:CH * q + CH], out)
        return out

    def unpack_sums(p):
        gq = lax.broadcasted_iota(jnp.int32, (CH, LANE), I1) // IMG
        rows = []
        for q in range(QUAD):
            z = jnp.where(gq == q, p, ZERO)
            z = z + pltpu.roll(z, IMG, I1)
            rows.append(z + pltpu.roll(z, HALFL, I1))
        return jnp.concatenate(rows, axis=I0)

    def reduce_copies(a):
        return [pltpu.make_async_remote_copy(
            src_ref=sa.at[a], dst_ref=ra.at[a, d - I1], send_sem=as_sem.at[a, d - I1], recv_sem=ar_sem.at[a, d - I1],
            device_id=peer(d), device_id_type=MESH) for d in range(I1, SUB)]

    def reduce_start(a):
        for c in reduce_copies(a):
            c.start()

    def reduce_finish(a):
        for c in reduce_copies(a):
            c.wait()
        total = sa[a]
        for d in range(TAP):
            total = total + ra[a, d]
        return total

    def build_band(way, k):
        diag = lax.rem(lax.broadcasted_iota(jnp.int32, (SUB, LANE), I1), SUB) == lax.broadcasted_iota(jnp.int32, (SUB, LANE), I0)

        def one(g, carry):
            base = jnp.concatenate([jnp.where(diag, jnp.broadcast_to(eb[way, g, i, k:k + I1, :], (SUB, LANE)), ZERO)
                                    for i in range(SUB)], axis=I1)
            for h in range(PAIR):
                for wp in range(QUAD):
                    rows = [pltpu.roll(base, h * LANE + (PAIR * wp + q + I1) * SUB, I1) for q in range(PAIR)]
                    at = (h * QUAD + wp) * PR
                    tbuf[g, at:at + PR, :] = jnp.concatenate(rows, axis=I0).astype(BF16)
            return carry
        lax.fori_loop(I0, NG, one, I0)

    def conv(src, finish):
        def step(hp, carry):
            for g in range(NG):
                tile = src[g, pl.ds(PAIR * hp, SUB)].reshape(BAND, PXL)
                finish(g, hp, dot(tbuf[g], tile))
            return carry
        lax.fori_loop(I0, RAD, step, I0)

    def load_pair(ref, i):
        return [ref[g, i].astype(F32).reshape(PAIR, SUB, PXL) for g in range(NG)]

    def to_mat(pieces):
        return jnp.concatenate([jnp.concatenate([p[q] for p in pieces], axis=I0) for q in range(PAIR)], axis=I1)

    def from_mat(m):
        return [jnp.concatenate([m[SUB * g:SUB * g + SUB, I0:PXL][None], m[SUB * g:SUB * g + SUB, PXL:PXP][None]], axis=I0)
                for g in range(NG)]

    def chan_mean(pieces):
        t = pieces[I0]
        for p in pieces[I1:]:
            t = t + p
        return jnp.sum(t, axis=I1, keepdims=True) * (ONE / 40.0)

    def norm_pair(k, i):
        d = [dbuf[k, g, i].astype(F32).reshape(PAIR, SUB, PXL) for g in range(NG)]
        mu = chan_mean(d)
        c = [v - mu for v in d]
        inv = lax.rsqrt(chan_mean([v * v for v in c]) + EPS)
        return [v * inv for v in c], inv

    def gelu_of(x):
        return (0.5 * x) * (ONE + lax.erf(x * 0.7071067811865476))

    def mask_row(k):
        m = mask[k, I0:I1, :]
        return jnp.concatenate([m, m], axis=I1)

    def conv_forward(k, src):
        bias = [col(k, CONVB + SUB * g, SUB, PXL) for g in range(NG)]

        def finish(g, hp, acc):
            v = acc.reshape(PR, SUB, PXL) + bias[g][None]
            dbuf[k, g, pl.ds(SUB * hp, SUB)] = v.reshape(SUB, PR, PXL).astype(BF16)
        conv(src, finish)

    def hidden_forward(k):
        acc_g2[...] = jnp.zeros_like(acc_g2)

        def step(i, carry):
            nrm, _ = norm_pair(k, i)
            n = [nrm[g] * col(k, NORMG + SUB * g, SUB, PXL)[None] + col(k, NORMB + SUB * g, SUB, PXL)[None] for g in range(NG)]
            n.append(jnp.ones((PAIR, SUB, PXL), F32))
            nb = to_mat(n).astype(BF16)
            nbuf[k, i] = nb
            h = (dot(w1t[k], nb) + col(k, FC1B, HID, PXP)).astype(BF16)
            hbuf[k, i] = h
            g = gelu_of(h.astype(F32))
            g = g * g
            acc_g2[...] += g[:, I0:PXL] + g[:, PXL:PXP]
            return carry
        lax.fori_loop(I0, NPAIR, step, I0)

    def scale_from(k, total):
        gn = jnp.sqrt(unpack_sums(total))
        mean = jnp.sum(gn, axis=I0, keepdims=True) * (ONE / 160.0) + EPS
        gnbuf[k] = gn
        sbuf[k] = cols[k, GAMMA:GAMMA + HID, :] * (gn / mean) + ONE

    def wide(v, width):
        return jnp.concatenate([v] * (width // LANE), axis=I1)

    def resp_of(k, g):
        return (g * wide(sbuf[k], PXP) + col(k, BETA, HID, PXP)).astype(BF16)

    def project(k, i, r, res):
        o = dot(w2t[k], r) + col(k, FC2B, CH, PXP)
        o = from_mat(o * mask_row(k))
        return [(res[g] + o[g]).reshape(PR, PXL).astype(BF16) for g in range(NG)]

    def block1_out():
        def step(i, carry):
            r = resp_of(I0, gelu_of(hbuf[I0, i].astype(F32)))
            hh, wp = i // QUAD, lax.rem(i, QUAD)
            res = [x1[g, RAD + hh, PAIR + wp].astype(F32).reshape(PAIR, SUB, PXL) for g in range(NG)]
            y = project(I0, i, r, res)
            for g in range(NG):
                x2[g, RAD + hh, PAIR + wp] = y[g]
            return carry
        lax.fori_loop(I0, NPAIR, step, I0)

    def cross_phase(k, dy):
        acc_cross[...] = jnp.zeros_like(acc_cross)
        acc_beta[...] = jnp.zeros_like(acc_beta)

        def step(i, carry):
            dm = to_mat(load_pair(dy, i)).astype(BF16)
            dr = (dot(w2[k], dm) * mask_row(k)).astype(BF16)
            drbuf[i] = dr
            dr = dr.astype(F32)
            cr = dr * gelu_of(hbuf[k, i].astype(F32))
            acc_cross[...] += cr[:, I0:PXL] + cr[:, PXL:PXP]
            acc_beta[...] += dr[:, I0:PXL] + dr[:, PXL:PXP]
            return carry
        lax.fori_loop(I0, NPAIR, step, I0)

    def grn_grad(k, total):
        gn = gnbuf[k]
        cross = unpack_sums(total)
        mean = jnp.sum(gn, axis=I0, keepdims=True) * (ONE / 160.0) + EPS
        ds = cols[k, GAMMA:GAMMA + HID, :] * cross
        dg = ds / mean - jnp.sum(ds * gn, axis=I0, keepdims=True) / (mean * mean * 160.0)
        qbuf[...] = dg / gn

    def hidden_backward(k, dy, with_out):
        acc_f1[...] = jnp.zeros_like(acc_f1)
        acc_f2[...] = jnp.zeros_like(acc_f2)
        acc_n[...] = jnp.zeros_like(acc_n)

        def step(i, carry):
            hh, wp = i // QUAD, lax.rem(i, QUAD)
            x = hbuf[k, i].astype(F32)
            phi = 0.5 + 0.5 * lax.erf(x * 0.7071067811865476)
            g = x * phi
            slope = phi + (x * 0.3989422804014327) * jnp.exp(-0.5 * (x * x))
            r = resp_of(k, g)
            if with_out:
                res = [x2[g_, RAD + hh, PAIR + wp].astype(F32).reshape(PAIR, SUB, PXL) for g_ in range(NG)]
                y = project(k, i, r, res)
                for g_ in range(NG):
                    y_out[g_, i] = y[g_]
            dm = to_mat(load_pair(dy, i))
            dz = jnp.where(mask_row(k) > ZERO, dm, ZERO)
            dz = jnp.concatenate([dz, jnp.zeros((SUB, PXP), F32)], axis=I0).astype(BF16)
            nb = nbuf[k, i]
            rhs = jnp.concatenate([nb, dz], axis=I0)
            dga = drbuf[i].astype(F32) * wide(sbuf[k], PXP) + g * wide(qbuf[...], PXP)
            dh = (dga * slope).astype(BF16)
            raug = jnp.concatenate([r, jnp.ones((PR, PXP), BF16)], axis=I0)
            acc_f1[...] += nt_dot(dh, rhs)
            acc_f2[...] += nt_dot(raug, rhs)
            dn = from_mat(dot(w1[k], dh).astype(BF16).astype(F32))
            nrm, inv = norm_pair(k, i)
            dx = [dn[g_] * col(k, NORMG + SUB * g_, SUB, PXL)[None] for g_ in range(NG)]
            m1 = chan_mean(dx)
            m2 = chan_mean([a * b for a, b in zip(dx, nrm)])
            for g_ in range(NG):
                dd = (inv * (dx[g_] - m1 - nrm[g_] * m2)).astype(BF16)
                dp[g_, RAD + hh, PAIR + wp] = dd.reshape(PR, PXL)
                dd = dd.astype(F32)
                pg = dn[g_] * nrm[g_]
                acc_n[I0, SUB * g_:SUB * g_ + SUB, :] += pg[I0] + pg[I1]
                acc_n[I1, SUB * g_:SUB * g_ + SUB, :] += dn[g_][I0] + dn[g_][I1]
                acc_n[PAIR, SUB * g_:SUB * g_ + SUB, :] += dd[I0] + dd[I1]
            return carry
        lax.fori_loop(I0, NPAIR, step, I0)

    def conv_wgrad(k, src):
        sub = lax.broadcasted_iota(jnp.int32, (SUB, BAND), I0)
        lane = lax.rem(lax.broadcasted_iota(jnp.int32, (SUB, BAND), I1), SUB)

        def one(g, carry):
            for hp in range(RAD):
                a = dp[g, RAD + PAIR * hp:NG + PAIR * hp, PAIR:TILEH].reshape(LANE, PXL)
                b = src[g, PAIR * hp:PAIR * hp + SUB].reshape(BAND, PXL)
                part = nt_dot(a, b)
                if hp == I0:
                    gvec[...] = part
                else:
                    gvec[...] += part
            out = jnp.zeros((SUB, BAND), F32)
            for h in range(PAIR):
                for w in range(SUB):
                    at = (h * SUB + w) * SUB
                    out = out + pltpu.roll(gvec[at:at + SUB, :], BAND - (h * LANE + (w + I1) * SUB), I1)
            out = jnp.sum(jnp.where(sub == lane, out, ZERO), axis=I0, keepdims=True)
            rows = jnp.concatenate([out[:, LANE * i:LANE * i + LANE] for i in range(SUB)], axis=I0)
            gb[k, pl.ds(HIDP + SUB * g, SUB), :] = rows
            return carry
        lax.fori_loop(I0, NG, one, I0)

    def store_grads(k):
        lane = lax.broadcasted_iota(jnp.int32, (HIDP, LANE), I1)
        f1 = jnp.concatenate([acc_f1[...], jnp.zeros((PR, TQ), F32)], axis=I0)
        f1 = jnp.concatenate([f1, jnp.zeros((HIDP, IMG), F32)], axis=I1)
        f2 = jnp.concatenate([acc_f2[...], jnp.zeros((HIDP, IMG), F32)], axis=I1)
        out = jnp.where(lane < CHP, f1, jnp.where(lane < CHQ, f2, ZERO))

        def column(v, lane_at, n):
            c = jnp.sum(v, axis=I1, keepdims=True)
            c = jnp.concatenate([c, jnp.zeros((HIDP - n, I1), F32)], axis=I0)
            return jnp.where(lane == lane_at, c, ZERO)
        gn = gnbuf[k]
        mean = jnp.sum(gn, axis=I0, keepdims=True) * (ONE / 160.0) + EPS
        out = out + column(acc_beta[:, I0:LANE] + acc_beta[:, LANE:PXL], CHQ, HID)
        out = out + column((acc_cross[:, I0:LANE] + acc_cross[:, LANE:PXL]) * (gn / mean), 89, HID)
        for j in range(RAD):
            out = out + column(acc_n[j, :, I0:LANE] + acc_n[j, :, LANE:PXL], 90 + j, CH)
        gb[k, I0:HIDP, :] = out
        gb[k, 216:224, :] = jnp.zeros((SUB, LANE), F32)

    def conv_backward(dy, out):
        def finish(g, hp, acc):
            v = acc.reshape(SUB, PR, PXL) + dy[g, pl.ds(SUB * hp, SUB)].astype(F32)
            out[g, pl.ds(SUB * hp, SUB)] = v.astype(BF16)
        conv(dp, finish)

    def to_x1(g, i, v):
        x1[g, RAD + i // QUAD, PAIR + lax.rem(i, QUAD)] = v

    def to_gout(g, i, v):
        gout[g, i] = v
    load_tiles(xin, to_x1)
    halo_start(x1, I0)
    setup()
    load_tiles(gin, to_gout)
    build_band(I0, I0)
    halo_finish(x1, I0)
    conv_forward(I0, x1)
    hidden_forward(I0)
    sa[I0, I0:CH] = pack_sums(fold(acc_g2))
    sa[I0, CH:80] = jnp.zeros((CH, LANE), F32)
    reduce_start(I0)
    build_band(I0, I1)
    total = reduce_finish(I0)
    scale_from(I0, total[I0:CH])
    block1_out()
    halo_start(x2, I1)
    halo_finish(x2, I1)
    conv_forward(I1, x2)
    hidden_forward(I1)
    cross_phase(I1, gout)
    sa[I1, I0:CH] = pack_sums(fold(acc_g2))
    sa[I1, CH:80] = pack_sums(fold(acc_cross))
    reduce_start(I1)
    build_band(I1, I1)
    total = reduce_finish(I1)
    scale_from(I1, total[I0:CH])
    grn_grad(I1, total[CH:80])
    hidden_backward(I1, gout, True)
    halo_start(dp, PAIR)
    conv_wgrad(I1, x2)
    store_grads(I1)
    halo_finish(dp, PAIR)
    conv_backward(gout, dmid)
    cross_phase(I0, dmid)
    sa[PAIR, I0:CH] = pack_sums(fold(acc_cross))
    sa[PAIR, CH:80] = jnp.zeros((CH, LANE), F32)
    reduce_start(PAIR)
    build_band(I1, I0)
    total = reduce_finish(PAIR)
    grn_grad(I0, total[I0:CH])
    hidden_backward(I0, dmid, False)
    halo_start(dp, RAD)
    conv_wgrad(I0, x1)
    store_grads(I0)
    halo_finish(dp, RAD)

    def part(f):
        return gb.at[f // QUAD, pl.ds(pl.multiple_of(lax.rem(f, QUAD) * 56, SUB), 56)]

    scat = [pltpu.make_async_remote_copy(
        src_ref=part(lax.rem(me + d, SUB)), dst_ref=grx.at[d - I1], send_sem=gs_sem.at[d - I1], recv_sem=gr_sem.at[d - I1],
        device_id=peer(d), device_id_type=MESH) for d in range(I1, SUB)]
    for c in scat:
        c.start()
    conv_backward(dmid, dx_out)
    for c in scat:
        c.wait()
    mine = gb[me // QUAD, pl.ds(pl.multiple_of(lax.rem(me, QUAD) * 56, SUB), 56), :]
    for d in range(TAP):
        mine = mine + grx[d]
    gs[TAP] = mine
    gath = [pltpu.make_async_remote_copy(
        src_ref=gs.at[TAP], dst_ref=gs.at[d - I1], send_sem=as2_sem.at[d - I1], recv_sem=ar2_sem.at[d - I1],
        device_id=peer(d), device_id_type=MESH) for d in range(I1, SUB)]
    for c in gath:
        c.start()
    for c in gath:
        c.wait()
    gr_out[me] = gs[TAP]
    for d in range(I1, SUB):
        gr_out[lax.rem(me + SUB - d, SUB)] = gs[d - I1]


def run_kernel(args):
    act = jax.ShapeDtypeStruct((NG, NPAIR, PR, PXL), BF16)
    vm = pl.BlockSpec(memory_space=pltpu.VMEM)
    pad = pltpu.VMEM((NG, PADH, SUB, PR, PXL), BF16)
    return pl.pallas_call(
        kernel,
        name='blocks',
        out_shape=(act, act, jax.ShapeDtypeStruct((SUB, 56, LANE), F32)),
        in_specs=[vm] * len(args),
        out_specs=(vm, vm, vm),
        scratch_shapes=[
            pltpu.VMEM((12288, CH), F32), pltpu.VMEM((NG, NPAIR, PR, PXL), BF16),
            pltpu.VMEM((PAIR, SUB, PXL), F32), pltpu.VMEM((PAIR, NG, SUB, SUB, LANE), F32), pltpu.VMEM((PAIR, 640, LANE), F32),
            pltpu.VMEM((PAIR, HID, CHP), BF16), pltpu.VMEM((PAIR, HID, CH), BF16),
            pad, pad, pad,
            pltpu.VMEM((PAIR, NG, NPAIR, PR, PXL), BF16),
            pltpu.VMEM((PAIR, NPAIR, CHP, PXP), BF16),
            pltpu.VMEM((PAIR, NPAIR, HID, PXP), BF16),
            pltpu.VMEM((NPAIR, HID, PXP), BF16),
            pltpu.VMEM((NG, NPAIR, PR, PXL), BF16),
            pltpu.VMEM((NG, LANE, BAND), BF16),
            pltpu.VMEM((HID, PXL), F32), pltpu.VMEM((HID, PXL), F32), pltpu.VMEM((HID, PXL), F32),
            pltpu.VMEM((RAD, CH, PXL), F32),
            pltpu.VMEM((HID, TQ), F32), pltpu.VMEM((HIDP, TQ), F32),
            pltpu.VMEM((LANE, BAND), F32),
            pltpu.VMEM((PAIR, HID, LANE), F32), pltpu.VMEM((PAIR, HID, LANE), F32), pltpu.VMEM((HID, LANE), F32),
            pltpu.VMEM((QUAD, NG, RAD, QUAD, PR, LANE), BF16), pltpu.VMEM((QUAD, NG, RAD, QUAD, PR, LANE), BF16),
            pltpu.VMEM((QUAD, 18, CH, LANE), BF16), pltpu.VMEM((QUAD, PADH, CH, LANE), BF16),
            pltpu.VMEM((RAD, 80, LANE), F32), pltpu.VMEM((RAD, TAP, 80, LANE), F32),
            pltpu.VMEM((PAIR, ROWS, LANE), F32), pltpu.VMEM((TAP, 56, LANE), F32), pltpu.VMEM((SUB, 56, LANE), F32),
            pltpu.SemaphoreType.DMA((QUAD, NG)), pltpu.SemaphoreType.DMA((QUAD, NG)),
            pltpu.SemaphoreType.DMA((RAD, TAP)), pltpu.SemaphoreType.DMA((RAD, TAP)),
            pltpu.SemaphoreType.DMA((TAP,)), pltpu.SemaphoreType.DMA((TAP,)),
            pltpu.SemaphoreType.DMA((TAP,)), pltpu.SemaphoreType.DMA((TAP,)),
        ],
        compiler_params=pltpu.CompilerParams(collective_id=I0, has_side_effects=True, vmem_limit_bytes=60 * PAIR**20),
    )(*args)


def finish_kernel(y, dx, gr, act_out, grad_in, o_taps, o_bconv, o_gnorm, o_bnorm, o_w1, o_b1, o_gamma, o_beta, o_w2, o_b2, yf):
    def unload(src, dst):
        def step(i, carry):
            first = (i // QUAD) * IMG + lax.rem(i, QUAD) * PAIR
            v = [src[g, i].astype(F32) for g in range(NG)]
            for q in range(PAIR):
                m = jnp.transpose(jnp.concatenate([p[SUB * q:SUB * q + SUB] for p in v], axis=I0))
                for j in range(SUB):
                    yf[pl.ds(first + (q + (j // QUAD) * 192 + (j % QUAD) * SUB), IMG, stride=PIX), :] = m[IMG * j:IMG * j + IMG]
            return carry
        lax.fori_loop(I0, NPAIR, step, I0)

        def narrow(b, carry):
            dst[b] = yf[pl.ds(pl.multiple_of(b * PIX, PIX), PIX), :].reshape(PADH, IMG, CH).astype(BF16)
            return carry
        lax.fori_loop(I0, IMG, narrow, I0)
    unload(y, act_out)
    unload(dx, grad_in)
    for k in range(PAIR):
        t = jnp.transpose(gr[k, I0:HID, :])
        o_w1[k] = t[I0:CH]
        o_w2[k] = t[CHP:CHQ] * KEEP
        o_b1[k:k + I1, :] = t[CH:41]
        o_beta[k:k + I1, :] = t[CHQ:89]
        o_gamma[k:k + I1, :] = t[89:90]
        o_gnorm[k:k + I1, :] = t[90:91, I0:CH]
        o_bnorm[k:k + I1, :] = t[91:92, I0:CH]
        o_bconv[k:k + I1, :] = t[92:93, I0:CH]
        o_b2[k:k + I1, :] = gr[k, HID:161, CHP:CHQ] * KEEP
    place = lax.broadcasted_iota(jnp.int32, (PAIR, LANE), I1) // SUB

    def taps_row(i, carry):
        for j in range(TAP):
            out = jnp.zeros((PAIR, LANE), F32)
            for g in range(NG):
                rows = jnp.concatenate([gr[k, pl.ds(HIDP + SUB * g + i, I1), :] for k in range(PAIR)], axis=I0)
                out = jnp.where(place == g, pltpu.roll(rows, (LANE + SUB * (g - j)) % LANE, I1), out)
            o_taps[i, j] = out[:, I0:CH]
        return carry
    lax.fori_loop(I0, TAP, taps_row, I0)


def finish(y, dx, gr):
    vm = pl.BlockSpec(memory_space=pltpu.VMEM)
    shape = lambda *s: jax.ShapeDtypeStruct(s, F32)
    act = jax.ShapeDtypeStruct((IMG, PADH, IMG, CH), BF16)
    small, wide = shape(PAIR, CH), shape(PAIR, HID)
    return pl.pallas_call(
        finish_kernel, name='finish',
        out_shape=(act, act, shape(TAP, TAP, PAIR, CH), small, small, small, shape(PAIR, CH, HID), wide, wide, wide, shape(PAIR, CH, HID), small),
        in_specs=[vm] * RAD, out_specs=(vm,) * PADH,
        scratch_shapes=[pltpu.VMEM((12288, CH), F32)],
        compiler_params=pltpu.CompilerParams(vmem_limit_bytes=CH * PAIR**20),
    )(y, dx, gr)


def solution(mesh):
    act_spec = P('dp', 'sh', 'sw', None)
    rep = P()

    def local_step(act_in, drop_mask, grad_out, conv_w, conv_b, norm_g, norm_b, fc1_w, fc1_b, grn_gamma, grn_beta, fc2_w, fc2_b):
        y, dx, gr = run_kernel((act_in, grad_out, drop_mask.T, conv_w.transpose(I1, PAIR, I0, RAD), fc1_b, grn_gamma, grn_beta,
                                conv_b, norm_g, norm_b, fc2_b, fc1_w, fc2_w.transpose(I0, PAIR, I1)))
        act_out, grad_in, taps, *rest = finish(y, dx, gr.reshape(PAIR, ROWS, LANE))
        rest[TAP] = rest[TAP].transpose(I0, PAIR, I1)
        return (act_out, grad_in, taps.transpose(PAIR, I0, I1, RAD), *rest)

    return jax.shard_map(local_step, mesh=mesh,
                         in_specs=(act_spec, P('dp', None), act_spec) + (rep,) * 10,
                         out_specs=(act_spec, act_spec) + (P('dp'),) * 10,
                         check_vma=False)
```

```python
import functools

import jax
import jax.numpy as jnp
import numpy as np
from jax import lax
from jax.experimental import pallas as pl
from jax.experimental.pallas import tpu as pltpu
from jax.sharding import PartitionSpec as P

EPS = 1e-6
F32 = jnp.float32
BF16 = jnp.bfloat16
MESH = pl.DeviceIdType.MESH
NG = 5
NPAIR = 24
ROWS = 224
KEEP = 4.0 / 3.0
FC1B, GAMMA, BETA, CONVB, NORMG, NORMB, FC2B = 0, 160, 320, 480, 520, 560, 600


LANE = 128
PXL = 256
PXP = 512
SUB = 8
CH = 40
HID = 160
IMG = 32
PR = 16
TQ = 96
CHP = 48
BAND = 1024
PIX = 384
HIDP = 176
CHQ = 88
HALFL = 64
PADH = 12
ZERO = 0.0
ONE = 1.0
TAP = 7
TILEH = 6
QUAD = 4
RAD = 3
PAIR = 2
I0 = 0
I1 = 1


def nt_dot(a, b):
    return lax.dot_general(a, b, (((I1,), (I1,)), ((), ())), preferred_element_type=F32)


def dot(a, b):
    return jnp.dot(a, b, preferred_element_type=F32)


def kernel(xin, gin, mask_in, taps, b_fc1, gamma, beta, b_conv, g_norm, b_norm, b_fc2, w1, w2t,
           y_out, dx_out, gr_out,
           xf, gout, mask, eb, cols, w1t, w2, x1, x2, dp, dbuf, nbuf, hbuf, drbuf, dmid, tbuf,
           acc_g2, acc_cross, acc_beta, acc_n, acc_f1, acc_f2, gvec, sbuf, gnbuf, qbuf,
           ru, rd, rc, sc, sa, ra, gb, grx, gs,
           hs_sem, hr_sem, as_sem, ar_sem, gs_sem, gr_sem, as2_sem, ar2_sem):
    sw = lax.axis_index('sw')
    sh = lax.axis_index('sh')
    me = sw * QUAD + sh
    other_w = I1 - sw

    def peer(d):
        f = lax.rem(me + d, SUB)
        return {'sw': f // QUAD, 'sh': lax.rem(f, QUAD)}

    barrier = pltpu.get_barrier_semaphore()
    for d in range(I1, SUB):
        pl.semaphore_signal(barrier, inc=I1, device_id=peer(d), device_id_type=MESH)
    pl.semaphore_wait(barrier, TAP)

    def setup():
        spots = ((b_fc1, FC1B), (gamma, GAMMA), (beta, BETA), (b_conv, CONVB),
                 (g_norm, NORMG), (b_norm, NORMB), (b_fc2, FC2B))
        for k in range(PAIR):
            for ref, at in spots:
                n = ref.shape[I1]
                row = jnp.broadcast_to(ref[k:k + I1, :], (LANE, n))
                cols[k, at:at + n, :] = jnp.transpose(row)
            m = jnp.concatenate([mask_in[k:k + I1, :]] * SUB, axis=I1)
            mask[k] = jnp.broadcast_to(m, (SUB, PXL))
            w1t[k] = jnp.transpose(jnp.concatenate([w1[k].astype(F32), jnp.zeros((SUB, HID), F32)], axis=I0)).astype(BF16)
            w2[k] = jnp.transpose(w2t[k].astype(F32)).astype(BF16)
        eb[...] = jnp.zeros_like(eb)
        place = lax.broadcasted_iota(jnp.int32, (PAIR, LANE), I1) // SUB

        def taps_row(i, carry):
            rows = [jnp.concatenate([taps[i, j].astype(F32), jnp.zeros((PAIR, CHQ), F32)], axis=I1) for j in range(TAP)]
            for g in range(NG):
                fwd = jnp.zeros((PAIR, LANE), F32)
                bwd = jnp.zeros((PAIR, LANE), F32)
                for j in range(TAP):
                    fwd = jnp.where(place == j, pltpu.roll(rows[j], (LANE + SUB * (j - g)) % LANE, I1), fwd)
                    bwd = jnp.where(place == TILEH - j, pltpu.roll(rows[j], (LANE + SUB * (TILEH - j - g)) % LANE, I1), bwd)
                eb[I0, g, i, I0:PAIR, :] = fwd
                eb[I1, g, TILEH - i, I0:PAIR, :] = bwd
            return carry
        lax.fori_loop(I0, TAP, taps_row, I0)

    def load_tiles(src, store):
        def widen(b, carry):
            xf[pl.ds(b * 385, PIX), :] = src[b].reshape(PIX, CH).astype(F32)
            return carry
        lax.fori_loop(I0, IMG, widen, I0, unroll=QUAD)
        unit = jnp.where(lax.broadcasted_iota(jnp.int32, (CH, CH), I0) == lax.broadcasted_iota(jnp.int32, (CH, CH), I1),
                         ONE, ZERO).astype(BF16)

        def step(i, carry):
            first = (i // QUAD) * IMG + lax.rem(i, QUAD) * PAIR
            px = []
            for q in range(PAIR):
                rows = [xf[pl.ds(first + (q + hb * 192 + wb * SUB), IMG, stride=385), :]
                        for hb in range(PAIR) for wb in range(QUAD)]
                px.append(nt_dot(unit, jnp.concatenate(rows, axis=I0).astype(BF16)))
            for g in range(NG):
                store(g, i, jnp.concatenate([p[SUB * g:SUB * g + SUB] for p in px], axis=I0).astype(BF16))
            return carry
        lax.fori_loop(I0, NPAIR, step, I0, unroll=QUAD)

    def col(k, off, n, width):
        piece = cols[k, off:off + n, :]
        return jnp.concatenate([piece] * (width // LANE), axis=I1)

    lane128 = lax.broadcasted_iota(jnp.int32, (SUB, LANE), I1)
    grp = lane128 // IMG

    def halo_copies(src, e):
        up = {'sw': sw, 'sh': jnp.maximum(sh - I1, I0)}
        down = {'sw': sw, 'sh': jnp.minimum(sh + I1, RAD)}
        upx = {'sw': other_w, 'sh': jnp.maximum(sh - I1, I0)}
        downx = {'sw': other_w, 'sh': jnp.minimum(sh + I1, RAD)}

        def cp(s, d, i, dev):
            return pltpu.make_async_remote_copy(
                src_ref=s, dst_ref=d, send_sem=hs_sem.at[e, i], recv_sem=hr_sem.at[e, i],
                device_id=dev, device_id_type=MESH)
        return (
            lambda: cp(src.at[:, TILEH:9, PAIR:TILEH, :, LANE:PXL], ru.at[e], I0, down),
            lambda: cp(src.at[:, RAD:TILEH, PAIR:TILEH, :, I0:LANE], rd.at[e], I1, up),
            lambda: cp(sc.at[e], rc.at[e, RAD:15], PAIR, {'sw': other_w, 'sh': sh}),
            lambda: cp(sc.at[e, 9:PADH], rc.at[e, I0:RAD], RAD, downx),
            lambda: cp(sc.at[e, I0:RAD], rc.at[e, 15:18], QUAD, upx),
        )

    def halo_start(src, e):
        copies = halo_copies(src, e)

        @pl.when(sh < RAD)
        def _():
            copies[I0]().start()

        @pl.when(sh > I0)
        def _():
            copies[I1]().start()
        first = QUAD - PAIR * sw

        def pack(h, carry):
            for half in range(PAIR):
                ls = slice(half * LANE, half * LANE + LANE)
                pieces = []
                for g in range(NG):
                    v = src[g, RAD + h, pl.ds(first, PAIR), :, ls].astype(F32).reshape(QUAD, SUB, LANE)
                    out = jnp.zeros((SUB, LANE), F32)
                    for q in range(QUAD):
                        shift = lax.rem(q * IMG + IMG * (I1 - sw), LANE)
                        out = jnp.where(grp == q, pltpu.roll(v[q], shift, I1), out)
                    pieces.append(out)
                sc[e, TILEH * half + h] = jnp.concatenate(pieces, axis=I0).astype(BF16)
            return carry
        lax.fori_loop(I0, TILEH, pack, I0, unroll=PAIR)
        copies[PAIR]().start()

        @pl.when(sh < RAD)
        def _():
            copies[RAD]().start()

        @pl.when(sh > I0)
        def _():
            copies[QUAD]().start()

        @pl.when(sh == I0)
        def _():
            ru[e] = jnp.zeros(ru.shape[I1:], BF16)
            rc[e, I0:RAD] = jnp.zeros((RAD, CH, LANE), BF16)

        @pl.when(sh == RAD)
        def _():
            rd[e] = jnp.zeros(rd.shape[I1:], BF16)
            rc[e, 15:18] = jnp.zeros((RAD, CH, LANE), BF16)

    def halo_finish(src, e):
        copies = halo_copies(src, e)

        @pl.when(sh < RAD)
        def _():
            copies[I0]().wait_send()
            copies[RAD]().wait_send()
            copies[I1]().wait_recv()
            copies[QUAD]().wait_recv()

        @pl.when(sh > I0)
        def _():
            copies[I1]().wait_send()
            copies[QUAD]().wait_send()
            copies[I0]().wait_recv()
            copies[RAD]().wait_recv()
        copies[PAIR]().wait()
        for r in range(RAD):
            src[:, r, PAIR:TILEH, :, LANE:PXL] = src[:, TILEH + r, PAIR:TILEH, :, I0:LANE]
            src[:, r, PAIR:TILEH, :, I0:LANE] = ru[e, :, r]
            src[:, 9 + r, PAIR:TILEH, :, I0:LANE] = src[:, RAD + r, PAIR:TILEH, :, LANE:PXL]
            src[:, 9 + r, PAIR:TILEH, :, LANE:PXL] = rd[e, :, r]
        is_left = (lane128 < IMG)
        is_right = (lane128 >= TQ)
        keep_left = jnp.where(sw == I1, ONE, ZERO)
        keep_right = jnp.where(sw == I0, ONE, ZERO)

        def pad(h, carry):
            for half in range(PAIR):
                ls = slice(half * LANE, half * LANE + LANE)
                strip = rc[e, h + TILEH * half].astype(F32).reshape(NG, SUB, LANE)
                for g in range(NG):
                    hi = src[g, h, QUAD:TILEH, :, ls].astype(F32).reshape(QUAD, SUB, LANE)
                    lo = src[g, h, PAIR:QUAD, :, ls].astype(F32).reshape(QUAD, SUB, LANE)
                    left, right = [], []
                    for q in range(QUAD):
                        shift = lax.rem(jnp.where(sw == I1, LANE - q * IMG, 224 - q * IMG), LANE)
                        edge = pltpu.roll(strip[g], shift, I1)
                        left.append(jnp.where(is_left, edge * keep_left, pltpu.roll(hi[q], IMG, I1)))
                        right.append(jnp.where(is_right, edge * keep_right, pltpu.roll(lo[q], TQ, I1)))
                    src[g, h, I0:PAIR, :, ls] = jnp.concatenate(left, axis=I0).reshape(PAIR, PR, LANE).astype(BF16)
                    src[g, h, TILEH:SUB, :, ls] = jnp.concatenate(right, axis=I0).reshape(PAIR, PR, LANE).astype(BF16)
            return carry
        lax.fori_loop(I0, PADH, pad, I0, unroll=PAIR)

    def fold(ref):
        v = ref[:, I0:LANE] + ref[:, LANE:PXL]
        v = v + pltpu.roll(v, IMG, I1)
        return v + pltpu.roll(v, HALFL, I1)

    def pack_sums(v):
        gq = lax.broadcasted_iota(jnp.int32, (CH, LANE), I1) // IMG
        out = v[I0:CH]
        for q in range(I1, QUAD):
            out = jnp.where(gq == q, v[CH * q:CH * q + CH], out)
        return out

    def unpack_sums(p):
        gq = lax.broadcasted_iota(jnp.int32, (CH, LANE), I1) // IMG
        rows = []
        for q in range(QUAD):
            z = jnp.where(gq == q, p, ZERO)
            z = z + pltpu.roll(z, IMG, I1)
            rows.append(z + pltpu.roll(z, HALFL, I1))
        return jnp.concatenate(rows, axis=I0)

    def reduce_copies(a, n):
        return [pltpu.make_async_remote_copy(
            src_ref=sa.at[a, I0:n], dst_ref=ra.at[a, d - I1, I0:n], send_sem=as_sem.at[a, d - I1], recv_sem=ar_sem.at[a, d - I1],
            device_id=peer(d), device_id_type=MESH) for d in range(I1, SUB)]

    def reduce_start(a, n):
        for c in reduce_copies(a, n):
            c.start()

    def reduce_finish(a, n):
        for c in reduce_copies(a, n):
            c.wait()
        total = sa[a, I0:n]
        for d in range(TAP):
            total = total + ra[a, d, I0:n]
        return total

    def build_band(way, k):
        diag = lax.rem(lax.broadcasted_iota(jnp.int32, (SUB, LANE), I1), SUB) == lax.broadcasted_iota(jnp.int32, (SUB, LANE), I0)

        def one(g, carry):
            base = jnp.concatenate([jnp.where(diag, jnp.broadcast_to(eb[way, g, i, k:k + I1, :], (SUB, LANE)), ZERO)
                                    for i in range(SUB)], axis=I1)
            for h in range(PAIR):
                for wp in range(QUAD):
                    rows = [pltpu.roll(base, h * LANE + (PAIR * wp + q + I1) * SUB, I1) for q in range(PAIR)]
                    at = (h * QUAD + wp) * PR
                    tbuf[g, at:at + PR, :] = jnp.concatenate(rows, axis=I0).astype(BF16)
            return carry
        lax.fori_loop(I0, NG, one, I0, unroll=NG)

    def conv(src, finish):
        def step(hp, carry):
            for g in range(NG):
                tile = src[g, pl.ds(PAIR * hp, SUB)].reshape(BAND, PXL)
                finish(g, hp, dot(tbuf[g], tile))
            return carry
        lax.fori_loop(I0, RAD, step, I0, unroll=RAD)

    def load_pair(ref, i):
        return [ref[g, i].astype(F32).reshape(PAIR, SUB, PXL) for g in range(NG)]

    def to_mat(pieces):
        return jnp.concatenate([jnp.concatenate([p[q] for p in pieces], axis=I0) for q in range(PAIR)], axis=I1)

    def from_mat(m):
        return [jnp.concatenate([m[SUB * g:SUB * g + SUB, I0:PXL][None], m[SUB * g:SUB * g + SUB, PXL:PXP][None]], axis=I0)
                for g in range(NG)]

    def chan_mean(pieces):
        t = pieces[I0]
        for p in pieces[I1:]:
            t = t + p
        return jnp.sum(t, axis=I1, keepdims=True) * (ONE / 40.0)

    def norm_pair(k, i):
        d = [dbuf[k, g, i].astype(F32).reshape(PAIR, SUB, PXL) for g in range(NG)]
        mu = chan_mean(d)
        c = [v - mu for v in d]
        inv = lax.rsqrt(chan_mean([v * v for v in c]) + EPS)
        return [v * inv for v in c], inv

    def gelu_of(x):
        return (0.5 * x) * (ONE + lax.erf(x * 0.7071067811865476))

    def mask_row(k):
        m = mask[k, I0:I1, :]
        return jnp.concatenate([m, m], axis=I1)

    def conv_forward(k, src):
        bias = [col(k, CONVB + SUB * g, SUB, PXL) for g in range(NG)]

        def finish(g, hp, acc):
            v = acc.reshape(PR, SUB, PXL) + bias[g][None]
            dbuf[k, g, pl.ds(SUB * hp, SUB)] = v.reshape(SUB, PR, PXL).astype(BF16)
        conv(src, finish)

    def hidden_forward(k, with_cross):
        acc_g2[...] = jnp.zeros_like(acc_g2)
        if with_cross:
            acc_cross[...] = jnp.zeros_like(acc_cross)

        def step(i, carry):
            nrm, _ = norm_pair(k, i)
            n = [nrm[g] * col(k, NORMG + SUB * g, SUB, PXL)[None] + col(k, NORMB + SUB * g, SUB, PXL)[None] for g in range(NG)]
            n.append(jnp.ones((PAIR, SUB, PXL), F32))
            nb = to_mat(n).astype(BF16)
            nbuf[k, i] = nb
            h = (dot(w1t[k], nb) + col(k, FC1B, HID, PXP)).astype(BF16)
            hbuf[k, i] = h
            g = gelu_of(h.astype(F32))
            if with_cross:
                cr = drbuf[i].astype(F32) * g
                acc_cross[...] += cr[:, I0:PXL] + cr[:, PXL:PXP]
            g = g * g
            acc_g2[...] += g[:, I0:PXL] + g[:, PXL:PXP]
            return carry
        lax.fori_loop(I0, NPAIR, step, I0, unroll=QUAD)

    def scale_from(k, total):
        gn = jnp.sqrt(unpack_sums(total))
        mean = jnp.sum(gn, axis=I0, keepdims=True) * (ONE / 160.0) + EPS
        gnbuf[k] = gn
        sbuf[k] = cols[k, GAMMA:GAMMA + HID, :] * (gn / mean) + ONE

    def wide(v, width):
        return jnp.concatenate([v] * (width // LANE), axis=I1)

    def resp_of(k, g):
        return (g * wide(sbuf[k], PXP) + col(k, BETA, HID, PXP)).astype(BF16)

    def project(k, i, r, res):
        o = dot(w2t[k], r) + col(k, FC2B, CH, PXP)
        o = from_mat(o * mask_row(k))
        return [(res[g] + o[g]).reshape(PR, PXL).astype(BF16) for g in range(NG)]

    def block1_out():
        def step(i, carry):
            r = resp_of(I0, gelu_of(hbuf[I0, i].astype(F32)))
            hh, wp = i // QUAD, lax.rem(i, QUAD)
            res = [x1[g, RAD + hh, PAIR + wp].astype(F32).reshape(PAIR, SUB, PXL) for g in range(NG)]
            y = project(I0, i, r, res)
            for g in range(NG):
                x2[g, RAD + hh, PAIR + wp] = y[g]
            return carry
        lax.fori_loop(I0, NPAIR, step, I0, unroll=QUAD)

    def resp_phase(k, dy, with_cross):
        if with_cross:
            acc_cross[...] = jnp.zeros_like(acc_cross)
        acc_beta[...] = jnp.zeros_like(acc_beta)

        def step(i, carry):
            dm = to_mat(load_pair(dy, i)).astype(BF16)
            dr = (dot(w2[k], dm) * mask_row(k)).astype(BF16)
            drbuf[i] = dr
            dr = dr.astype(F32)
            if with_cross:
                cr = dr * gelu_of(hbuf[k, i].astype(F32))
                acc_cross[...] += cr[:, I0:PXL] + cr[:, PXL:PXP]
            acc_beta[...] += dr[:, I0:PXL] + dr[:, PXL:PXP]
            return carry
        lax.fori_loop(I0, NPAIR, step, I0, unroll=QUAD)

    def grn_grad(k, total):
        gn = gnbuf[k]
        cross = unpack_sums(total)
        mean = jnp.sum(gn, axis=I0, keepdims=True) * (ONE / 160.0) + EPS
        ds = cols[k, GAMMA:GAMMA + HID, :] * cross
        dg = ds / mean - jnp.sum(ds * gn, axis=I0, keepdims=True) / (mean * mean * 160.0)
        qbuf[...] = dg / gn

    def hidden_backward(k, dy, with_out):
        acc_f1[...] = jnp.zeros_like(acc_f1)
        acc_f2[...] = jnp.zeros_like(acc_f2)
        acc_n[...] = jnp.zeros_like(acc_n)

        def step(i, carry):
            hh, wp = i // QUAD, lax.rem(i, QUAD)
            x = hbuf[k, i].astype(F32)
            phi = 0.5 + 0.5 * lax.erf(x * 0.7071067811865476)
            g = x * phi
            slope = phi + (x * 0.3989422804014327) * jnp.exp(-0.5 * (x * x))
            r = resp_of(k, g)
            if with_out:
                res = [x2[g_, RAD + hh, PAIR + wp].astype(F32).reshape(PAIR, SUB, PXL) for g_ in range(NG)]
                y = project(k, i, r, res)
                for g_ in range(NG):
                    y_out[g_, i] = y[g_]
            dm = to_mat(load_pair(dy, i))
            dz = jnp.where(mask_row(k) > ZERO, dm, ZERO)
            dz = jnp.concatenate([dz, jnp.zeros((SUB, PXP), F32)], axis=I0).astype(BF16)
            nb = nbuf[k, i]
            rhs = jnp.concatenate([nb, dz], axis=I0)
            dga = drbuf[i].astype(F32) * wide(sbuf[k], PXP) + g * wide(qbuf[...], PXP)
            dh = (dga * slope).astype(BF16)
            raug = jnp.concatenate([r, jnp.ones((PR, PXP), BF16)], axis=I0)
            acc_f1[...] += nt_dot(dh, rhs)
            acc_f2[...] += nt_dot(raug, rhs)
            dn = from_mat(dot(w1[k], dh).astype(BF16).astype(F32))
            nrm, inv = norm_pair(k, i)
            dx = [dn[g_] * col(k, NORMG + SUB * g_, SUB, PXL)[None] for g_ in range(NG)]
            m1 = chan_mean(dx)
            m2 = chan_mean([a * b for a, b in zip(dx, nrm)])
            for g_ in range(NG):
                dd = (inv * (dx[g_] - m1 - nrm[g_] * m2)).astype(BF16)
                dp[g_, RAD + hh, PAIR + wp] = dd.reshape(PR, PXL)
                dd = dd.astype(F32)
                pg = dn[g_] * nrm[g_]
                acc_n[I0, SUB * g_:SUB * g_ + SUB, :] += pg[I0] + pg[I1]
                acc_n[I1, SUB * g_:SUB * g_ + SUB, :] += dn[g_][I0] + dn[g_][I1]
                acc_n[PAIR, SUB * g_:SUB * g_ + SUB, :] += dd[I0] + dd[I1]
            return carry
        lax.fori_loop(I0, NPAIR, step, I0, unroll=QUAD)

    def conv_wgrad(k, src):
        sub = lax.broadcasted_iota(jnp.int32, (SUB, BAND), I0)
        lane = lax.rem(lax.broadcasted_iota(jnp.int32, (SUB, BAND), I1), SUB)

        def one(g, carry):
            for hp in range(RAD):
                a = dp[g, RAD + PAIR * hp:NG + PAIR * hp, PAIR:TILEH].reshape(LANE, PXL)
                b = src[g, PAIR * hp:PAIR * hp + SUB].reshape(BAND, PXL)
                part = nt_dot(a, b)
                if hp == I0:
                    gvec[...] = part
                else:
                    gvec[...] += part
            out = jnp.zeros((SUB, BAND), F32)
            for h in range(PAIR):
                for w in range(SUB):
                    at = (h * SUB + w) * SUB
                    out = out + pltpu.roll(gvec[at:at + SUB, :], BAND - (h * LANE + (w + I1) * SUB), I1)
            out = jnp.sum(jnp.where(sub == lane, out, ZERO), axis=I0, keepdims=True)
            rows = jnp.concatenate([out[:, LANE * i:LANE * i + LANE] for i in range(SUB)], axis=I0)
            gb[k, pl.ds(HIDP + SUB * g, SUB), :] = rows
            return carry
        lax.fori_loop(I0, NG, one, I0, unroll=NG)

    def store_grads(k):
        lane = lax.broadcasted_iota(jnp.int32, (HIDP, LANE), I1)
        f1 = jnp.concatenate([acc_f1[...], jnp.zeros((PR, TQ), F32)], axis=I0)
        f1 = jnp.concatenate([f1, jnp.zeros((HIDP, IMG), F32)], axis=I1)
        f2 = jnp.concatenate([acc_f2[...], jnp.zeros((HIDP, IMG), F32)], axis=I1)
        out = jnp.where(lane < CHP, f1, jnp.where(lane < CHQ, f2, ZERO))

        def column(v, lane_at, n):
            c = jnp.sum(v, axis=I1, keepdims=True)
            c = jnp.concatenate([c, jnp.zeros((HIDP - n, I1), F32)], axis=I0)
            return jnp.where(lane == lane_at, c, ZERO)
        gn = gnbuf[k]
        mean = jnp.sum(gn, axis=I0, keepdims=True) * (ONE / 160.0) + EPS
        out = out + column(acc_beta[:, I0:LANE] + acc_beta[:, LANE:PXL], CHQ, HID)
        out = out + column((acc_cross[:, I0:LANE] + acc_cross[:, LANE:PXL]) * (gn / mean), 89, HID)
        for j in range(RAD):
            out = out + column(acc_n[j, :, I0:LANE] + acc_n[j, :, LANE:PXL], 90 + j, CH)
        gb[k, I0:HIDP, :] = out
        gb[k, 216:224, :] = jnp.zeros((SUB, LANE), F32)

    def conv_backward(dy, out):
        def finish(g, hp, acc):
            v = acc.reshape(SUB, PR, PXL) + dy[g, pl.ds(SUB * hp, SUB)].astype(F32)
            out[g, pl.ds(SUB * hp, SUB)] = v.astype(BF16)
        conv(dp, finish)

    def to_x1(g, i, v):
        x1[g, RAD + i // QUAD, PAIR + lax.rem(i, QUAD)] = v

    def to_gout(g, i, v):
        gout[g, i] = v
    load_tiles(xin, to_x1)
    halo_start(x1, I0)
    setup()
    build_band(I0, I0)
    halo_finish(x1, I0)
    conv_forward(I0, x1)
    hidden_forward(I0, False)
    sa[I0, I0:CH] = pack_sums(fold(acc_g2))
    reduce_start(I0, CH)
    load_tiles(gin, to_gout)
    build_band(I0, I1)
    total = reduce_finish(I0, CH)
    scale_from(I0, total)
    block1_out()
    halo_start(x2, I1)
    resp_phase(I1, gout, False)
    halo_finish(x2, I1)
    conv_forward(I1, x2)
    hidden_forward(I1, True)
    sa[I1, I0:CH] = pack_sums(fold(acc_g2))
    sa[I1, CH:80] = pack_sums(fold(acc_cross))
    reduce_start(I1, 80)
    build_band(I1, I1)
    total = reduce_finish(I1, 80)
    scale_from(I1, total[I0:CH])
    grn_grad(I1, total[CH:80])
    hidden_backward(I1, gout, True)
    halo_start(dp, PAIR)
    conv_wgrad(I1, x2)
    store_grads(I1)
    halo_finish(dp, PAIR)
    conv_backward(gout, dmid)
    resp_phase(I0, dmid, True)
    sa[PAIR, I0:CH] = pack_sums(fold(acc_cross))
    reduce_start(PAIR, CH)
    build_band(I1, I0)
    total = reduce_finish(PAIR, CH)
    grn_grad(I0, total)
    hidden_backward(I0, dmid, False)
    halo_start(dp, RAD)
    conv_wgrad(I0, x1)
    store_grads(I0)

    def part(f):
        return gb.at[f // QUAD, pl.ds(pl.multiple_of(lax.rem(f, QUAD) * 56, SUB), 56)]

    scat = [pltpu.make_async_remote_copy(
        src_ref=part(lax.rem(me + d, SUB)), dst_ref=grx.at[d - I1], send_sem=gs_sem.at[d - I1], recv_sem=gr_sem.at[d - I1],
        device_id=peer(d), device_id_type=MESH) for d in range(I1, SUB)]
    for c in scat:
        c.start()
    halo_finish(dp, RAD)
    conv_backward(dmid, dx_out)
    for c in scat:
        c.wait()
    mine = gb[me // QUAD, pl.ds(pl.multiple_of(lax.rem(me, QUAD) * 56, SUB), 56), :]
    for d in range(TAP):
        mine = mine + grx[d]
    gs[TAP] = mine
    gath = [pltpu.make_async_remote_copy(
        src_ref=gs.at[TAP], dst_ref=gs.at[d - I1], send_sem=as2_sem.at[d - I1], recv_sem=ar2_sem.at[d - I1],
        device_id=peer(d), device_id_type=MESH) for d in range(I1, SUB)]
    for c in gath:
        c.start()
    for c in gath:
        c.wait()
    gr_out[me] = gs[TAP]
    for d in range(I1, SUB):
        gr_out[lax.rem(me + SUB - d, SUB)] = gs[d - I1]


def run_kernel(args):
    act = jax.ShapeDtypeStruct((NG, NPAIR, PR, PXL), BF16)
    vm = pl.BlockSpec(memory_space=pltpu.VMEM)
    pad = pltpu.VMEM((NG, PADH, SUB, PR, PXL), BF16)
    return pl.pallas_call(
        kernel,
        name='blocks',
        out_shape=(act, act, jax.ShapeDtypeStruct((SUB, 56, LANE), F32)),
        in_specs=[vm] * len(args),
        out_specs=(vm, vm, vm),
        scratch_shapes=[
            pltpu.VMEM((IMG * 385, CH), F32), pltpu.VMEM((NG, NPAIR, PR, PXL), BF16),
            pltpu.VMEM((PAIR, SUB, PXL), F32), pltpu.VMEM((PAIR, NG, SUB, SUB, LANE), F32), pltpu.VMEM((PAIR, 640, LANE), F32),
            pltpu.VMEM((PAIR, HID, CHP), BF16), pltpu.VMEM((PAIR, HID, CH), BF16),
            pad, pad, pad,
            pltpu.VMEM((PAIR, NG, NPAIR, PR, PXL), BF16),
            pltpu.VMEM((PAIR, NPAIR, CHP, PXP), BF16),
            pltpu.VMEM((PAIR, NPAIR, HID, PXP), BF16),
            pltpu.VMEM((NPAIR, HID, PXP), BF16),
            pltpu.VMEM((NG, NPAIR, PR, PXL), BF16),
            pltpu.VMEM((NG, LANE, BAND), BF16),
            pltpu.VMEM((HID, PXL), F32), pltpu.VMEM((HID, PXL), F32), pltpu.VMEM((HID, PXL), F32),
            pltpu.VMEM((RAD, CH, PXL), F32),
            pltpu.VMEM((HID, TQ), F32), pltpu.VMEM((HIDP, TQ), F32),
            pltpu.VMEM((LANE, BAND), F32),
            pltpu.VMEM((PAIR, HID, LANE), F32), pltpu.VMEM((PAIR, HID, LANE), F32), pltpu.VMEM((HID, LANE), F32),
            pltpu.VMEM((QUAD, NG, RAD, QUAD, PR, LANE), BF16), pltpu.VMEM((QUAD, NG, RAD, QUAD, PR, LANE), BF16),
            pltpu.VMEM((QUAD, 18, CH, LANE), BF16), pltpu.VMEM((QUAD, PADH, CH, LANE), BF16),
            pltpu.VMEM((RAD, 80, LANE), F32), pltpu.VMEM((RAD, TAP, 80, LANE), F32),
            pltpu.VMEM((PAIR, ROWS, LANE), F32), pltpu.VMEM((TAP, 56, LANE), F32), pltpu.VMEM((SUB, 56, LANE), F32),
            pltpu.SemaphoreType.DMA((QUAD, NG)), pltpu.SemaphoreType.DMA((QUAD, NG)),
            pltpu.SemaphoreType.DMA((RAD, TAP)), pltpu.SemaphoreType.DMA((RAD, TAP)),
            pltpu.SemaphoreType.DMA((TAP,)), pltpu.SemaphoreType.DMA((TAP,)),
            pltpu.SemaphoreType.DMA((TAP,)), pltpu.SemaphoreType.DMA((TAP,)),
        ],
        compiler_params=pltpu.CompilerParams(collective_id=I0, has_side_effects=True, vmem_limit_bytes=60 * PAIR**20),
    )(*args)


def finish_kernel(y, dx, gr, act_out, grad_in, o_taps, o_bconv, o_gnorm, o_bnorm, o_w1, o_b1, o_gamma, o_beta, o_w2, o_b2, yf):
    def unload(src, dst, n):
        for wp in range(QUAD):
            v = [src[g, wp].astype(F32) for g in range(NG)]
            for q in range(PAIR):
                m = jnp.transpose(jnp.concatenate([p[SUB * q:SUB * q + SUB] for p in v], axis=I0))
                for j in range(SUB):
                    at = (j // QUAD) * 1056 + (j % QUAD) * SUB + PAIR * wp + q
                    yf[n, pl.ds(at, IMG, stride=33), :] = m[IMG * j:IMG * j + IMG]
        for hb in range(PAIR):
            for b in range(IMG):
                at = hb * 1056 + b * 33
                dst[b, hb, I0] = yf[n, at:at + IMG, :].astype(BF16)
    unload(y, act_out, I0)
    unload(dx, grad_in, I1)

    @pl.when(pl.program_id(I0) == I0)
    def _():
        for k in range(PAIR):
            t = jnp.transpose(gr[k, I0:HID, :])
            o_w1[k] = t[I0:CH]
            o_w2[k] = t[CHP:CHQ] * KEEP
            o_b1[k:k + I1, :] = t[CH:41]
            o_beta[k:k + I1, :] = t[CHQ:89]
            o_gamma[k:k + I1, :] = t[89:90]
            o_gnorm[k:k + I1, :] = t[90:91, I0:CH]
            o_bnorm[k:k + I1, :] = t[91:92, I0:CH]
            o_bconv[k:k + I1, :] = t[92:93, I0:CH]
            o_b2[k:k + I1, :] = gr[k, HID:161, CHP:CHQ] * KEEP
        place = lax.broadcasted_iota(jnp.int32, (PAIR, LANE), I1) // SUB

        def taps_row(i, carry):
            for j in range(TAP):
                out = jnp.zeros((PAIR, LANE), F32)
                for g in range(NG):
                    rows = jnp.concatenate([gr[k, pl.ds(HIDP + SUB * g + i, I1), :] for k in range(PAIR)], axis=I0)
                    out = jnp.where(place == g, pltpu.roll(rows, (LANE + SUB * (g - j)) % LANE, I1), out)
                o_taps[i, j] = out[:, I0:CH]
            return carry
        lax.fori_loop(I0, TAP, taps_row, I0)


def finish(y, dx, gr):
    shape = lambda *d: jax.ShapeDtypeStruct(d, F32)
    act = jax.ShapeDtypeStruct((IMG, PAIR, TILEH, IMG, CH), BF16)
    small, wide = shape(PAIR, CH), shape(PAIR, HID)
    tile = pl.BlockSpec((NG, QUAD, PR, PXL), lambda h: (I0, h, I0, I0))
    rows = pl.BlockSpec((IMG, PAIR, I1, IMG, CH), lambda h: (I0, I0, h, I0, I0))
    whole = lambda o: pl.BlockSpec(o.shape, lambda h: (I0,) * len(o.shape))
    grads = (shape(TAP, TAP, PAIR, CH), small, small, small, shape(PAIR, CH, HID), wide, wide, wide, shape(PAIR, CH, HID), small)
    return pl.pallas_call(
        finish_kernel, name='finish', grid=(TILEH,),
        out_shape=(act, act) + grads,
        in_specs=[tile, tile, whole(gr)], out_specs=(rows, rows) + tuple(whole(o) for o in grads),
        scratch_shapes=[pltpu.VMEM((PAIR, 2112, CH), F32)],
        compiler_params=pltpu.CompilerParams(vmem_limit_bytes=60 * PAIR**20),
    )(y, dx, gr)


def solution(mesh):
    act_spec = P('dp', 'sh', 'sw', None)
    rep = P()

    def local_step(act_in, drop_mask, grad_out, conv_w, conv_b, norm_g, norm_b, fc1_w, fc1_b, grn_gamma, grn_beta, fc2_w, fc2_b):
        y, dx, gr = run_kernel((act_in, grad_out, drop_mask.T, conv_w.transpose(I1, PAIR, I0, RAD), fc1_b, grn_gamma, grn_beta,
                                conv_b, norm_g, norm_b, fc2_b, fc1_w, fc2_w.transpose(I0, PAIR, I1)))
        act_out, grad_in, taps, *rest = finish(y, dx, gr.reshape(PAIR, ROWS, LANE))
        rest[TAP] = rest[TAP].transpose(I0, PAIR, I1)
        return (act_out.reshape(IMG, PADH, IMG, CH), grad_in.reshape(IMG, PADH, IMG, CH), taps.transpose(PAIR, I0, I1, RAD), *rest)

    return jax.shard_map(local_step, mesh=mesh,
                         in_specs=(act_spec, P('dp', None), act_spec) + (rep,) * 10,
                         out_specs=(act_spec, act_spec) + (P('dp'),) * 10,
                         check_vma=False)
```

```python
import functools

import jax
import jax.numpy as jnp
import numpy as np
from jax import lax
from jax.experimental import pallas as pl
from jax.experimental.pallas import tpu as pltpu
from jax.sharding import PartitionSpec as P

EPS = 1e-6
F32 = jnp.float32
BF16 = jnp.bfloat16
MESH = pl.DeviceIdType.MESH
NG = 5
NPAIR = 24
ROWS = 224
KEEP = 4.0 / 3.0
FC1B, GAMMA, BETA, CONVB, NORMG, NORMB, FC2B = 0, 160, 320, 480, 520, 560, 600


LANE = 128
PXL = 256
PXP = 512
SUB = 8
CH = 40
HID = 160
IMG = 32
PR = 16
TQ = 96
CHP = 48
BAND = 1024
HIDP = 176
CHQ = 88
HALFL = 64
PADH = 12
ZERO = 0.0
ONE = 1.0
TAP = 7
TILEH = 6
QUAD = 4
RAD = 3
PAIR = 2
I0 = 0
I1 = 1


def nt_dot(a, b):
    return lax.dot_general(a, b, (((I1,), (I1,)), ((), ())), preferred_element_type=F32)


def dot(a, b):
    return jnp.dot(a, b, preferred_element_type=F32)


def kernel(xin, gin, mask_in, taps, b_fc1, gamma, beta, b_conv, g_norm, b_norm, b_fc2, w1, w2t,
           act_out, grad_in, o_taps, o_bconv, o_gnorm, o_bnorm, o_w1, o_b1, o_gamma, o_beta, o_w2, o_b2,
           io, xf, gout, ytile, mask, eb, cols, w1t, w2, x1, x2, dp, dbuf, nbuf, hbuf, g0buf, slbuf, drbuf, dmid, tbuf,
           acc_g2, acc_cross, acc_beta, acc_n, acc_f1, acc_f2, gvec, sbuf, gnbuf, qbuf,
           ru, rd, rc, sc, sa, ra, gb, grx, gs, grf,
           io_sem, hs_sem, hr_sem, as_sem, ar_sem, gs_sem, gr_sem, as2_sem, ar2_sem):
    sw = lax.axis_index('sw')
    sh = lax.axis_index('sh')
    me = sw * QUAD + sh
    other_w = I1 - sw

    def peer(d):
        f = lax.rem(me + d, SUB)
        return {'sw': f // QUAD, 'sh': lax.rem(f, QUAD)}

    barrier = pltpu.get_barrier_semaphore()
    for d in range(I1, SUB):
        pl.semaphore_signal(barrier, inc=I1, device_id=peer(d), device_id_type=MESH)

    def setup():
        spots = ((b_fc1, FC1B), (gamma, GAMMA), (beta, BETA), (b_conv, CONVB),
                 (g_norm, NORMG), (b_norm, NORMB), (b_fc2, FC2B))
        for k in range(PAIR):
            for ref, at in spots:
                n = ref.shape[I1]
                row = jnp.broadcast_to(ref[k:k + I1, :], (LANE, n))
                cols[k, at:at + n, :] = jnp.transpose(row)
            m = jnp.concatenate([mask_in[k:k + I1, :]] * SUB, axis=I1)
            mask[k] = jnp.broadcast_to(m, (SUB, PXL))
            w1t[k] = jnp.transpose(jnp.concatenate([w1[k].astype(F32), jnp.zeros((SUB, HID), F32)], axis=I0)).astype(BF16)
            w2[k] = jnp.transpose(w2t[k].astype(F32)).astype(BF16)
        eb[...] = jnp.zeros_like(eb)
        place = lax.broadcasted_iota(jnp.int32, (PAIR, LANE), I1) // SUB

        def taps_row(i, carry):
            rows = [jnp.concatenate([taps[i, j].astype(F32), jnp.zeros((PAIR, CHQ), F32)], axis=I1) for j in range(TAP)]
            for g in range(NG):
                fwd = jnp.zeros((PAIR, LANE), F32)
                bwd = jnp.zeros((PAIR, LANE), F32)
                for j in range(TAP):
                    fwd = jnp.where(place == j, pltpu.roll(rows[j], (LANE + SUB * (j - g)) % LANE, I1), fwd)
                    bwd = jnp.where(place == TILEH - j, pltpu.roll(rows[j], (LANE + SUB * (TILEH - j - g)) % LANE, I1), bwd)
                eb[I0, g, i, I0:PAIR, :] = fwd
                eb[I1, g, TILEH - i, I0:PAIR, :] = bwd
            return carry
        lax.fori_loop(I0, TAP, taps_row, I0)

    def fetch(src, c):
        return pltpu.make_async_copy(src.at[SUB * c:SUB * c + SUB], io.at[SUB * c:SUB * c + SUB], io_sem.at[c])

    def load_tiles(store):
        unit = jnp.where(lax.broadcasted_iota(jnp.int32, (CH, CH), I0) == lax.broadcasted_iota(jnp.int32, (CH, CH), I1),
                         ONE, ZERO).astype(BF16)

        def step(h, carry):
            for hb in range(PAIR):
                for b in range(IMG):
                    at = hb * 1056 + b * 33
                    xf[at:at + IMG, :] = io[b, hb * TILEH + h].astype(F32)
            for wp in range(QUAD):
                px = []
                for q in range(PAIR):
                    rows = [xf[pl.ds(hb * 1056 + wb * SUB + PAIR * wp + q, IMG, stride=33), :]
                            for hb in range(PAIR) for wb in range(QUAD)]
                    px.append(nt_dot(unit, jnp.concatenate(rows, axis=I0).astype(BF16)))
                for g in range(NG):
                    store(g, h, wp, jnp.concatenate([p[SUB * g:SUB * g + SUB] for p in px], axis=I0).astype(BF16))
            return carry
        lax.fori_loop(I0, TILEH, step, I0)

    def put(dst, h, hb):
        return pltpu.make_async_copy(io.at[:, hb * TILEH + h], dst.at[:, hb * TILEH + h], io_sem.at[h + TILEH * hb])

    def unload_tiles(src, dst):
        def step(h, carry):
            for wp in range(QUAD):
                v = [src[g, QUAD * h + wp].astype(F32) for g in range(NG)]
                for q in range(PAIR):
                    m = jnp.transpose(jnp.concatenate([p[SUB * q:SUB * q + SUB] for p in v], axis=I0))
                    for j in range(SUB):
                        at = (j // QUAD) * 1056 + (j % QUAD) * SUB + PAIR * wp + q
                        xf[pl.ds(at, IMG, stride=33), :] = m[IMG * j:IMG * j + IMG]
            for hb in range(PAIR):
                for b in range(IMG):
                    at = hb * 1056 + b * 33
                    io[b, hb * TILEH + h] = xf[at:at + IMG, :].astype(BF16)
                put(dst, h, hb).start()
            return carry
        lax.fori_loop(I0, TILEH, step, I0)

    def unload_wait(dst):
        for h in range(TILEH):
            for hb in range(PAIR):
                put(dst, h, hb).wait()

    def col(k, off, n, width):
        piece = cols[k, off:off + n, :]
        return jnp.concatenate([piece] * (width // LANE), axis=I1)

    lane128 = lax.broadcasted_iota(jnp.int32, (SUB, LANE), I1)
    grp = lane128 // IMG

    def halo_copies(src, e):
        up = {'sw': sw, 'sh': jnp.maximum(sh - I1, I0)}
        down = {'sw': sw, 'sh': jnp.minimum(sh + I1, RAD)}
        upx = {'sw': other_w, 'sh': jnp.maximum(sh - I1, I0)}
        downx = {'sw': other_w, 'sh': jnp.minimum(sh + I1, RAD)}

        def cp(s, d, i, dev):
            return pltpu.make_async_remote_copy(
                src_ref=s, dst_ref=d, send_sem=hs_sem.at[e, i], recv_sem=hr_sem.at[e, i],
                device_id=dev, device_id_type=MESH)
        return (
            lambda: cp(src.at[:, TILEH:9, PAIR:TILEH, :, LANE:PXL], ru.at[e], I0, down),
            lambda: cp(src.at[:, RAD:TILEH, PAIR:TILEH, :, I0:LANE], rd.at[e], I1, up),
            lambda: cp(sc.at[e], rc.at[e, RAD:15], PAIR, {'sw': other_w, 'sh': sh}),
            lambda: cp(sc.at[e, 9:PADH], rc.at[e, I0:RAD], RAD, downx),
            lambda: cp(sc.at[e, I0:RAD], rc.at[e, 15:18], QUAD, upx),
        )

    def halo_start(src, e):
        copies = halo_copies(src, e)

        @pl.when(sh < RAD)
        def _():
            copies[I0]().start()

        @pl.when(sh > I0)
        def _():
            copies[I1]().start()
        first = QUAD - PAIR * sw

        def pack(h, carry):
            for half in range(PAIR):
                ls = slice(half * LANE, half * LANE + LANE)
                pieces = []
                for g in range(NG):
                    v = src[g, RAD + h, pl.ds(first, PAIR), :, ls].astype(F32).reshape(QUAD, SUB, LANE)
                    out = jnp.zeros((SUB, LANE), F32)
                    for q in range(QUAD):
                        shift = lax.rem(q * IMG + IMG * (I1 - sw), LANE)
                        out = jnp.where(grp == q, pltpu.roll(v[q], shift, I1), out)
                    pieces.append(out)
                sc[e, TILEH * half + h] = jnp.concatenate(pieces, axis=I0).astype(BF16)
            return carry
        lax.fori_loop(I0, TILEH, pack, I0, unroll=PAIR)
        copies[PAIR]().start()

        @pl.when(sh < RAD)
        def _():
            copies[RAD]().start()

        @pl.when(sh > I0)
        def _():
            copies[QUAD]().start()

        @pl.when(sh == I0)
        def _():
            ru[e] = jnp.zeros(ru.shape[I1:], BF16)
            rc[e, I0:RAD] = jnp.zeros((RAD, CH, LANE), BF16)

        @pl.when(sh == RAD)
        def _():
            rd[e] = jnp.zeros(rd.shape[I1:], BF16)
            rc[e, 15:18] = jnp.zeros((RAD, CH, LANE), BF16)

    def halo_finish(src, e):
        copies = halo_copies(src, e)

        @pl.when(sh < RAD)
        def _():
            copies[I0]().wait_send()
            copies[RAD]().wait_send()
            copies[I1]().wait_recv()
            copies[QUAD]().wait_recv()

        @pl.when(sh > I0)
        def _():
            copies[I1]().wait_send()
            copies[QUAD]().wait_send()
            copies[I0]().wait_recv()
            copies[RAD]().wait_recv()
        copies[PAIR]().wait()
        for r in range(RAD):
            src[:, r, PAIR:TILEH, :, LANE:PXL] = src[:, TILEH + r, PAIR:TILEH, :, I0:LANE]
            src[:, r, PAIR:TILEH, :, I0:LANE] = ru[e, :, r]
            src[:, 9 + r, PAIR:TILEH, :, I0:LANE] = src[:, RAD + r, PAIR:TILEH, :, LANE:PXL]
            src[:, 9 + r, PAIR:TILEH, :, LANE:PXL] = rd[e, :, r]
        is_left = (lane128 < IMG)
        is_right = (lane128 >= TQ)
        keep_left = jnp.where(sw == I1, ONE, ZERO)
        keep_right = jnp.where(sw == I0, ONE, ZERO)

        def pad(h, carry):
            for half in range(PAIR):
                ls = slice(half * LANE, half * LANE + LANE)
                strip = rc[e, h + TILEH * half].astype(F32).reshape(NG, SUB, LANE)
                for g in range(NG):
                    hi = src[g, h, QUAD:TILEH, :, ls].astype(F32).reshape(QUAD, SUB, LANE)
                    lo = src[g, h, PAIR:QUAD, :, ls].astype(F32).reshape(QUAD, SUB, LANE)
                    left, right = [], []
                    for q in range(QUAD):
                        shift = lax.rem(jnp.where(sw == I1, LANE - q * IMG, 224 - q * IMG), LANE)
                        edge = pltpu.roll(strip[g], shift, I1)
                        left.append(jnp.where(is_left, edge * keep_left, pltpu.roll(hi[q], IMG, I1)))
                        right.append(jnp.where(is_right, edge * keep_right, pltpu.roll(lo[q], TQ, I1)))
                    src[g, h, I0:PAIR, :, ls] = jnp.concatenate(left, axis=I0).reshape(PAIR, PR, LANE).astype(BF16)
                    src[g, h, TILEH:SUB, :, ls] = jnp.concatenate(right, axis=I0).reshape(PAIR, PR, LANE).astype(BF16)
            return carry
        lax.fori_loop(I0, PADH, pad, I0, unroll=PAIR)

    def fold(ref):
        v = ref[:, I0:LANE] + ref[:, LANE:PXL]
        v = v + pltpu.roll(v, IMG, I1)
        return v + pltpu.roll(v, HALFL, I1)

    def pack_sums(v):
        gq = lax.broadcasted_iota(jnp.int32, (CH, LANE), I1) // IMG
        out = v[I0:CH]
        for q in range(I1, QUAD):
            out = jnp.where(gq == q, v[CH * q:CH * q + CH], out)
        return out

    def unpack_sums(p):
        gq = lax.broadcasted_iota(jnp.int32, (CH, LANE), I1) // IMG
        rows = []
        for q in range(QUAD):
            z = jnp.where(gq == q, p, ZERO)
            z = z + pltpu.roll(z, IMG, I1)
            rows.append(z + pltpu.roll(z, HALFL, I1))
        return jnp.concatenate(rows, axis=I0)

    def reduce_copies(a, n):
        return [pltpu.make_async_remote_copy(
            src_ref=sa.at[a, I0:n], dst_ref=ra.at[a, d - I1, I0:n], send_sem=as_sem.at[a, d - I1], recv_sem=ar_sem.at[a, d - I1],
            device_id=peer(d), device_id_type=MESH) for d in range(I1, SUB)]

    def reduce_start(a, n):
        for c in reduce_copies(a, n):
            c.start()

    def reduce_finish(a, n):
        for c in reduce_copies(a, n):
            c.wait()
        total = sa[a, I0:n]
        for d in range(TAP):
            total = total + ra[a, d, I0:n]
        return total

    def build_band(way, k):
        diag = lax.rem(lax.broadcasted_iota(jnp.int32, (SUB, LANE), I1), SUB) == lax.broadcasted_iota(jnp.int32, (SUB, LANE), I0)

        def one(g, carry):
            base = jnp.concatenate([jnp.where(diag, jnp.broadcast_to(eb[way, g, i, k:k + I1, :], (SUB, LANE)), ZERO)
                                    for i in range(SUB)], axis=I1)
            for h in range(PAIR):
                for wp in range(QUAD):
                    rows = [pltpu.roll(base, h * LANE + (PAIR * wp + q + I1) * SUB, I1) for q in range(PAIR)]
                    at = (h * QUAD + wp) * PR
                    tbuf[g, at:at + PR, :] = jnp.concatenate(rows, axis=I0).astype(BF16)
            return carry
        lax.fori_loop(I0, NG, one, I0, unroll=NG)

    def conv(src, finish):
        def step(hp, carry):
            for g in range(NG):
                tile = src[g, pl.ds(PAIR * hp, SUB)].reshape(BAND, PXL)
                finish(g, hp, dot(tbuf[g], tile))
            return carry
        lax.fori_loop(I0, RAD, step, I0, unroll=RAD)

    def load_pair(ref, i):
        return [ref[g, i].astype(F32).reshape(PAIR, SUB, PXL) for g in range(NG)]

    def to_mat(pieces):
        return jnp.concatenate([jnp.concatenate([p[q] for p in pieces], axis=I0) for q in range(PAIR)], axis=I1)

    def from_mat(m):
        return [jnp.concatenate([m[SUB * g:SUB * g + SUB, I0:PXL][None], m[SUB * g:SUB * g + SUB, PXL:PXP][None]], axis=I0)
                for g in range(NG)]

    def chan_mean(pieces):
        t = pieces[I0]
        for p in pieces[I1:]:
            t = t + p
        return jnp.sum(t, axis=I1, keepdims=True) * (ONE / 40.0)

    def norm_pair(k, i):
        d = [dbuf[k, g, i].astype(F32).reshape(PAIR, SUB, PXL) for g in range(NG)]
        mu = chan_mean(d)
        c = [v - mu for v in d]
        inv = lax.rsqrt(chan_mean([v * v for v in c]) + EPS)
        return [v * inv for v in c], inv

    def gelu_of(x):
        return (0.5 * x) * (ONE + lax.erf(x * 0.7071067811865476))

    def mask_row(k):
        m = mask[k, I0:I1, :]
        return jnp.concatenate([m, m], axis=I1)

    def conv_forward(k, src):
        bias = [col(k, CONVB + SUB * g, SUB, PXL) for g in range(NG)]

        def finish(g, hp, acc):
            v = acc.reshape(PR, SUB, PXL) + bias[g][None]
            dbuf[k, g, pl.ds(SUB * hp, SUB)] = v.reshape(SUB, PR, PXL).astype(BF16)
        conv(src, finish)

    def hidden_forward(k, with_cross):
        acc_g2[...] = jnp.zeros_like(acc_g2)
        if with_cross:
            acc_cross[...] = jnp.zeros_like(acc_cross)

        def step(i, carry):
            nrm, _ = norm_pair(k, i)
            n = [nrm[g] * col(k, NORMG + SUB * g, SUB, PXL)[None] + col(k, NORMB + SUB * g, SUB, PXL)[None] for g in range(NG)]
            n.append(jnp.ones((PAIR, SUB, PXL), F32))
            nb = to_mat(n).astype(BF16)
            nbuf[k, i] = nb
            h = (dot(w1t[k], nb) + col(k, FC1B, HID, PXP)).astype(BF16)
            hbuf[k, i] = h
            g = gelu_of(h.astype(F32))
            if k == I0:
                g0buf[i] = g
            if with_cross:
                cr = drbuf[i].astype(F32) * g
                acc_cross[...] += cr[:, I0:PXL] + cr[:, PXL:PXP]
            g = g * g
            acc_g2[...] += g[:, I0:PXL] + g[:, PXL:PXP]
            return carry
        lax.fori_loop(I0, NPAIR, step, I0, unroll=QUAD)

    def scale_from(k, total):
        gn = jnp.sqrt(unpack_sums(total))
        mean = jnp.sum(gn, axis=I0, keepdims=True) * (ONE / 160.0) + EPS
        gnbuf[k] = gn
        sbuf[k] = cols[k, GAMMA:GAMMA + HID, :] * (gn / mean) + ONE

    def wide(v, width):
        return jnp.concatenate([v] * (width // LANE), axis=I1)

    def resp_of(k, g):
        return (g * wide(sbuf[k], PXP) + col(k, BETA, HID, PXP)).astype(BF16)

    def project(k, i, r, res):
        o = dot(w2t[k], r) + col(k, FC2B, CH, PXP)
        o = from_mat(o * mask_row(k))
        return [(res[g] + o[g]).reshape(PR, PXL).astype(BF16) for g in range(NG)]

    def block1_out():
        def step(i, carry):
            r = resp_of(I0, g0buf[i])
            hh, wp = i // QUAD, lax.rem(i, QUAD)
            res = [x1[g, RAD + hh, PAIR + wp].astype(F32).reshape(PAIR, SUB, PXL) for g in range(NG)]
            y = project(I0, i, r, res)
            for g in range(NG):
                x2[g, RAD + hh, PAIR + wp] = y[g]
            return carry
        lax.fori_loop(I0, NPAIR, step, I0, unroll=QUAD)

    def resp_phase(k, dy, with_cross):
        if with_cross:
            acc_cross[...] = jnp.zeros_like(acc_cross)
        acc_beta[...] = jnp.zeros_like(acc_beta)

        def step(i, carry):
            dm = to_mat(load_pair(dy, i)).astype(BF16)
            dr = (dot(w2[k], dm) * mask_row(k)).astype(BF16)
            drbuf[i] = dr
            dr = dr.astype(F32)
            if with_cross:
                cr = dr * g0buf[i]
                acc_cross[...] += cr[:, I0:PXL] + cr[:, PXL:PXP]
            acc_beta[...] += dr[:, I0:PXL] + dr[:, PXL:PXP]
            return carry
        lax.fori_loop(I0, NPAIR, step, I0, unroll=QUAD)

    def slope_phase(k):
        def step(i, carry):
            x = hbuf[k, i].astype(F32)
            phi = 0.5 + 0.5 * lax.erf(x * 0.7071067811865476)
            slbuf[i] = phi + (x * 0.3989422804014327) * jnp.exp(-0.5 * (x * x))
            return carry
        lax.fori_loop(I0, NPAIR, step, I0, unroll=QUAD)

    def grn_grad(k, total):
        gn = gnbuf[k]
        cross = unpack_sums(total)
        mean = jnp.sum(gn, axis=I0, keepdims=True) * (ONE / 160.0) + EPS
        ds = cols[k, GAMMA:GAMMA + HID, :] * cross
        dg = ds / mean - jnp.sum(ds * gn, axis=I0, keepdims=True) / (mean * mean * 160.0)
        qbuf[...] = dg / gn

    def hidden_backward(k, dy, with_out):
        acc_f1[...] = jnp.zeros_like(acc_f1)
        acc_f2[...] = jnp.zeros_like(acc_f2)
        acc_n[...] = jnp.zeros_like(acc_n)

        def step(i, carry):
            hh, wp = i // QUAD, lax.rem(i, QUAD)
            g = gelu_of(hbuf[k, i].astype(F32)) if k == I1 else g0buf[i]
            r = resp_of(k, g)
            if with_out:
                res = [x2[g_, RAD + hh, PAIR + wp].astype(F32).reshape(PAIR, SUB, PXL) for g_ in range(NG)]
                y = project(k, i, r, res)
                for g_ in range(NG):
                    ytile[g_, i] = y[g_]
            dm = to_mat(load_pair(dy, i))
            dz = jnp.where(mask_row(k) > ZERO, dm, ZERO)
            dz = jnp.concatenate([dz, jnp.zeros((SUB, PXP), F32)], axis=I0).astype(BF16)
            nb = nbuf[k, i]
            rhs = jnp.concatenate([nb, dz], axis=I0)
            dga = drbuf[i].astype(F32) * wide(sbuf[k], PXP) + g * wide(qbuf[...], PXP)
            dh = (dga * slbuf[i]).astype(BF16)
            raug = jnp.concatenate([r, jnp.ones((PR, PXP), BF16)], axis=I0)
            acc_f1[...] += nt_dot(dh, rhs)
            acc_f2[...] += nt_dot(raug, rhs)
            dn = from_mat(dot(w1[k], dh).astype(BF16).astype(F32))
            nrm, inv = norm_pair(k, i)
            dx = [dn[g_] * col(k, NORMG + SUB * g_, SUB, PXL)[None] for g_ in range(NG)]
            m1 = chan_mean(dx)
            m2 = chan_mean([a * b for a, b in zip(dx, nrm)])
            for g_ in range(NG):
                dd = (inv * (dx[g_] - m1 - nrm[g_] * m2)).astype(BF16)
                dp[g_, RAD + hh, PAIR + wp] = dd.reshape(PR, PXL)
                dd = dd.astype(F32)
                pg = dn[g_] * nrm[g_]
                acc_n[I0, SUB * g_:SUB * g_ + SUB, :] += pg[I0] + pg[I1]
                acc_n[I1, SUB * g_:SUB * g_ + SUB, :] += dn[g_][I0] + dn[g_][I1]
                acc_n[PAIR, SUB * g_:SUB * g_ + SUB, :] += dd[I0] + dd[I1]
            return carry
        lax.fori_loop(I0, NPAIR, step, I0, unroll=QUAD)

    def conv_wgrad(k, src):
        sub = lax.broadcasted_iota(jnp.int32, (SUB, BAND), I0)
        lane = lax.rem(lax.broadcasted_iota(jnp.int32, (SUB, BAND), I1), SUB)

        def one(g, carry):
            for hp in range(RAD):
                a = dp[g, RAD + PAIR * hp:NG + PAIR * hp, PAIR:TILEH].reshape(LANE, PXL)
                b = src[g, PAIR * hp:PAIR * hp + SUB].reshape(BAND, PXL)
                part = nt_dot(a, b)
                if hp == I0:
                    gvec[...] = part
                else:
                    gvec[...] += part
            out = jnp.zeros((SUB, BAND), F32)
            for h in range(PAIR):
                for w in range(SUB):
                    at = (h * SUB + w) * SUB
                    out = out + pltpu.roll(gvec[at:at + SUB, :], BAND - (h * LANE + (w + I1) * SUB), I1)
            out = jnp.sum(jnp.where(sub == lane, out, ZERO), axis=I0, keepdims=True)
            rows = jnp.concatenate([out[:, LANE * i:LANE * i + LANE] for i in range(SUB)], axis=I0)
            gb[k, pl.ds(HIDP + SUB * g, SUB), :] = rows
            return carry
        lax.fori_loop(I0, NG, one, I0, unroll=NG)

    def store_grads(k):
        lane = lax.broadcasted_iota(jnp.int32, (HIDP, LANE), I1)
        f1 = jnp.concatenate([acc_f1[...], jnp.zeros((PR, TQ), F32)], axis=I0)
        f1 = jnp.concatenate([f1, jnp.zeros((HIDP, IMG), F32)], axis=I1)
        f2 = jnp.concatenate([acc_f2[...], jnp.zeros((HIDP, IMG), F32)], axis=I1)
        out = jnp.where(lane < CHP, f1, jnp.where(lane < CHQ, f2, ZERO))

        def column(v, lane_at, n):
            c = jnp.sum(v, axis=I1, keepdims=True)
            c = jnp.concatenate([c, jnp.zeros((HIDP - n, I1), F32)], axis=I0)
            return jnp.where(lane == lane_at, c, ZERO)
        gn = gnbuf[k]
        mean = jnp.sum(gn, axis=I0, keepdims=True) * (ONE / 160.0) + EPS
        out = out + column(acc_beta[:, I0:LANE] + acc_beta[:, LANE:PXL], CHQ, HID)
        out = out + column((acc_cross[:, I0:LANE] + acc_cross[:, LANE:PXL]) * (gn / mean), 89, HID)
        for j in range(RAD):
            out = out + column(acc_n[j, :, I0:LANE] + acc_n[j, :, LANE:PXL], 90 + j, CH)
        gb[k, I0:HIDP, :] = out
        gb[k, 216:224, :] = jnp.zeros((SUB, LANE), F32)

    def conv_backward(dy, out):
        def finish(g, hp, acc):
            v = acc.reshape(SUB, PR, PXL) + dy[g, pl.ds(SUB * hp, SUB)].astype(F32)
            out[g, pl.ds(SUB * hp, SUB)] = v.astype(BF16)
        conv(dp, finish)

    def to_x1(g, h, wp, v):
        x1[g, RAD + h, PAIR + wp] = v

    def to_gout(g, h, wp, v):
        gout[g, QUAD * h + wp] = v
    for c in range(QUAD):
        fetch(xin, c).start()
    for c in range(QUAD):
        fetch(xin, c).wait()
    load_tiles(to_x1)
    for c in range(QUAD):
        fetch(gin, c).start()
    pl.semaphore_wait(barrier, TAP)
    halo_start(x1, I0)
    setup()
    build_band(I0, I0)
    halo_finish(x1, I0)
    conv_forward(I0, x1)
    hidden_forward(I0, False)
    sa[I0, I0:CH] = pack_sums(fold(acc_g2))
    reduce_start(I0, CH)
    for c in range(QUAD):
        fetch(gin, c).wait()
    load_tiles(to_gout)
    build_band(I0, I1)
    total = reduce_finish(I0, CH)
    scale_from(I0, total)
    block1_out()
    halo_start(x2, I1)
    resp_phase(I1, gout, False)
    halo_finish(x2, I1)
    conv_forward(I1, x2)
    hidden_forward(I1, True)
    sa[I1, I0:CH] = pack_sums(fold(acc_g2))
    sa[I1, CH:80] = pack_sums(fold(acc_cross))
    reduce_start(I1, 80)
    build_band(I1, I1)
    slope_phase(I1)
    total = reduce_finish(I1, 80)
    scale_from(I1, total[I0:CH])
    grn_grad(I1, total[CH:80])
    hidden_backward(I1, gout, True)
    halo_start(dp, PAIR)
    conv_wgrad(I1, x2)
    store_grads(I1)
    unload_tiles(ytile, act_out)
    halo_finish(dp, PAIR)
    conv_backward(gout, dmid)
    resp_phase(I0, dmid, True)
    sa[PAIR, I0:CH] = pack_sums(fold(acc_cross))
    reduce_start(PAIR, CH)
    build_band(I1, I0)
    slope_phase(I0)
    total = reduce_finish(PAIR, CH)
    grn_grad(I0, total)
    hidden_backward(I0, dmid, False)
    halo_start(dp, RAD)
    conv_wgrad(I0, x1)
    store_grads(I0)

    def part(f):
        return gb.at[f // QUAD, pl.ds(pl.multiple_of(lax.rem(f, QUAD) * 56, SUB), 56)]

    scat = [pltpu.make_async_remote_copy(
        src_ref=part(lax.rem(me + d, SUB)), dst_ref=grx.at[d - I1], send_sem=gs_sem.at[d - I1], recv_sem=gr_sem.at[d - I1],
        device_id=peer(d), device_id_type=MESH) for d in range(I1, SUB)]
    for c in scat:
        c.start()
    halo_finish(dp, RAD)
    conv_backward(dmid, dmid)
    for c in scat:
        c.wait()
    mine = gb[me // QUAD, pl.ds(pl.multiple_of(lax.rem(me, QUAD) * 56, SUB), 56), :]
    for d in range(TAP):
        mine = mine + grx[d]
    gs[TAP] = mine
    gath = [pltpu.make_async_remote_copy(
        src_ref=gs.at[TAP], dst_ref=gs.at[d - I1], send_sem=as2_sem.at[d - I1], recv_sem=ar2_sem.at[d - I1],
        device_id=peer(d), device_id_type=MESH) for d in range(I1, SUB)]
    for c in gath:
        c.start()
    unload_wait(act_out)
    unload_tiles(dmid, grad_in)
    for c in gath:
        c.wait()
    grf[me] = gs[TAP]
    for d in range(I1, SUB):
        grf[lax.rem(me + SUB - d, SUB)] = gs[d - I1]
    for k in range(PAIR):
        gb[k] = grf[QUAD * k:QUAD * k + QUAD].reshape(ROWS, LANE)
    for k in range(PAIR):
        t = jnp.transpose(gb[k, I0:HID, :])
        o_w1[k] = t[I0:CH]
        o_w2[k] = t[CHP:CHQ] * KEEP
        o_b1[k:k + I1, :] = t[CH:41]
        o_beta[k:k + I1, :] = t[CHQ:89]
        o_gamma[k:k + I1, :] = t[89:90]
        o_gnorm[k:k + I1, :] = t[90:91, I0:CH]
        o_bnorm[k:k + I1, :] = t[91:92, I0:CH]
        o_bconv[k:k + I1, :] = t[92:93, I0:CH]
        o_b2[k:k + I1, :] = gb[k, HID:161, CHP:CHQ] * KEEP
    place = lax.broadcasted_iota(jnp.int32, (PAIR, LANE), I1) // SUB

    def taps_row(i, carry):
        for j in range(TAP):
            out = jnp.zeros((PAIR, LANE), F32)
            for g in range(NG):
                rows = jnp.concatenate([gb[k, pl.ds(HIDP + SUB * g + i, I1), :] for k in range(PAIR)], axis=I0)
                out = jnp.where(place == g, pltpu.roll(rows, (LANE + SUB * (g - j)) % LANE, I1), out)
            o_taps[i, j] = out[:, I0:CH]
        return carry
    lax.fori_loop(I0, TAP, taps_row, I0)
    unload_wait(grad_in)


def run_kernel(args):
    vm = pl.BlockSpec(memory_space=pltpu.VMEM)
    hbm = pl.BlockSpec(memory_space=pl.ANY)
    pad = pltpu.VMEM((NG, PADH, SUB, PR, PXL), BF16)
    tiles = pltpu.VMEM((NG, NPAIR, PR, PXL), BF16)
    return pl.pallas_call(
        kernel,
        name='blocks',
        out_shape=out_shapes(),
        in_specs=[hbm] * PAIR + [vm] * (len(args) - PAIR),
        out_specs=(hbm,) * PAIR + (vm,) * 10,
        scratch_shapes=[
            pltpu.VMEM((IMG, PADH, IMG, CH), BF16), pltpu.VMEM((2112, CH), F32), tiles, tiles,
            pltpu.VMEM((PAIR, SUB, PXL), F32), pltpu.VMEM((PAIR, NG, SUB, SUB, LANE), F32), pltpu.VMEM((PAIR, 640, LANE), F32),
            pltpu.VMEM((PAIR, HID, CHP), BF16), pltpu.VMEM((PAIR, HID, CH), BF16),
            pad, pad, pad,
            pltpu.VMEM((PAIR, NG, NPAIR, PR, PXL), BF16),
            pltpu.VMEM((PAIR, NPAIR, CHP, PXP), BF16),
            pltpu.VMEM((PAIR, NPAIR, HID, PXP), BF16),
            pltpu.VMEM((NPAIR, HID, PXP), F32), pltpu.VMEM((NPAIR, HID, PXP), F32),
            pltpu.VMEM((NPAIR, HID, PXP), BF16),
            pltpu.VMEM((NG, NPAIR, PR, PXL), BF16),
            pltpu.VMEM((NG, LANE, BAND), BF16),
            pltpu.VMEM((HID, PXL), F32), pltpu.VMEM((HID, PXL), F32), pltpu.VMEM((HID, PXL), F32),
            pltpu.VMEM((RAD, CH, PXL), F32),
            pltpu.VMEM((HID, TQ), F32), pltpu.VMEM((HIDP, TQ), F32),
            pltpu.VMEM((LANE, BAND), F32),
            pltpu.VMEM((PAIR, HID, LANE), F32), pltpu.VMEM((PAIR, HID, LANE), F32), pltpu.VMEM((HID, LANE), F32),
            pltpu.VMEM((QUAD, NG, RAD, QUAD, PR, LANE), BF16), pltpu.VMEM((QUAD, NG, RAD, QUAD, PR, LANE), BF16),
            pltpu.VMEM((QUAD, 18, CH, LANE), BF16), pltpu.VMEM((QUAD, PADH, CH, LANE), BF16),
            pltpu.VMEM((RAD, 80, LANE), F32), pltpu.VMEM((RAD, TAP, 80, LANE), F32),
            pltpu.VMEM((PAIR, ROWS, LANE), F32), pltpu.VMEM((TAP, 56, LANE), F32), pltpu.VMEM((SUB, 56, LANE), F32), pltpu.VMEM((SUB, 56, LANE), F32),
            pltpu.SemaphoreType.DMA((PADH,)),
            pltpu.SemaphoreType.DMA((QUAD, NG)), pltpu.SemaphoreType.DMA((QUAD, NG)),
            pltpu.SemaphoreType.DMA((RAD, TAP)), pltpu.SemaphoreType.DMA((RAD, TAP)),
            pltpu.SemaphoreType.DMA((TAP,)), pltpu.SemaphoreType.DMA((TAP,)),
            pltpu.SemaphoreType.DMA((TAP,)), pltpu.SemaphoreType.DMA((TAP,)),
        ],
        compiler_params=pltpu.CompilerParams(collective_id=I0, has_side_effects=True, vmem_limit_bytes=67043328),
    )(*args)


def out_shapes():
    shape = lambda *d: jax.ShapeDtypeStruct(d, F32)
    act = jax.ShapeDtypeStruct((IMG, PADH, IMG, CH), BF16)
    small, wide = shape(PAIR, CH), shape(PAIR, HID)
    return (act, act, shape(TAP, TAP, PAIR, CH), small, small, small, shape(PAIR, CH, HID), wide, wide, wide, shape(PAIR, CH, HID), small)


def finish_kernel(*refs):
    n = len(refs) // RAD
    src, dst, mid = refs[I0:n], refs[n:PAIR * n], refs[PAIR * n:RAD * n]
    in_sem, out_sem = refs[RAD * n:]
    moves = []
    for a in range(n):
        cuts = [slice(SUB * c, SUB * c + SUB) for c in range(QUAD)] if a < PAIR else [slice(None)]
        for cut in cuts:
            moves.append((src[a].at[cut], mid[a].at[cut], dst[a].at[cut]))
    ins = [pltpu.make_async_copy(m[I0], m[I1], in_sem.at[c]) for c, m in enumerate(moves)]
    outs = [pltpu.make_async_copy(m[I1], m[PAIR], out_sem.at[c]) for c, m in enumerate(moves)]
    for c in ins:
        c.start()
    for c, o in zip(ins, outs):
        c.wait()
        o.start()
    for o in outs:
        o.wait()


def finish(parts):
    n = len(parts)
    hbm = pl.BlockSpec(memory_space=pl.ANY)
    return pl.pallas_call(
        finish_kernel, name='finish', out_shape=out_shapes(),
        in_specs=[hbm] * n, out_specs=(hbm,) * n,
        scratch_shapes=[pltpu.VMEM(o.shape, o.dtype) for o in out_shapes()] + [pltpu.SemaphoreType.DMA((n + TILEH,))] * PAIR,
        compiler_params=pltpu.CompilerParams(vmem_limit_bytes=67043328),
    )(*parts)


def solution(mesh):
    act_spec = P('dp', 'sh', 'sw', None)
    rep = P()

    def local_step(act_in, drop_mask, grad_out, conv_w, conv_b, norm_g, norm_b, fc1_w, fc1_b, grn_gamma, grn_beta, fc2_w, fc2_b):
        parts = run_kernel((act_in, grad_out, drop_mask.T, conv_w.transpose(I1, PAIR, I0, RAD), fc1_b, grn_gamma, grn_beta,
                            conv_b, norm_g, norm_b, fc2_b, fc1_w, fc2_w.transpose(I0, PAIR, I1)))
        act_out, grad_in, taps, *rest = finish(parts)
        rest[TAP] = rest[TAP].transpose(I0, PAIR, I1)
        return (act_out, grad_in, taps.transpose(PAIR, I0, I1, RAD), *rest)

    return jax.shard_map(local_step, mesh=mesh,
                         in_specs=(act_spec, P('dp', None), act_spec) + (rep,) * 10,
                         out_specs=(act_spec, act_spec) + (P('dp'),) * 10,
                         check_vma=False)
```

```python
import functools

import jax
import jax.numpy as jnp
import numpy as np
from jax import lax
from jax.experimental import pallas as pl
from jax.experimental.pallas import tpu as pltpu
from jax.sharding import PartitionSpec as P

EPS = 1e-6
F32 = jnp.float32
BF16 = jnp.bfloat16
MESH = pl.DeviceIdType.MESH
NG = 5
NPAIR = 24
ROWS = 224
KEEP = 4.0 / 3.0
FC1B, GAMMA, BETA, CONVB, NORMG, NORMB, FC2B = 0, 160, 320, 480, 520, 560, 600


LANE = 128
PXL = 256
PXP = 512
SUB = 8
CH = 40
HID = 160
IMG = 32
PR = 16
TQ = 96
CHP = 48
BAND = 1024
HIDP = 176
CHQ = 88
HALFL = 64
PADH = 12
ZERO = 0.0
ONE = 1.0
TAP = 7
TILEH = 6
QUAD = 4
RAD = 3
PAIR = 2
I0 = 0
I1 = 1


def nt_dot(a, b):
    return lax.dot_general(a, b, (((I1,), (I1,)), ((), ())), preferred_element_type=F32)


def dot(a, b):
    return jnp.dot(a, b, preferred_element_type=F32)


def kernel(xin, gin, mask_in, taps, b_fc1, gamma, beta, b_conv, g_norm, b_norm, b_fc2, w1, w2t,
           act_out, grad_in, o_taps, o_bconv, o_gnorm, o_bnorm, o_w1, o_b1, o_gamma, o_beta, o_w2, o_b2,
           io, xf, gout, ytile, mask, eb, cols, w1t, w2, x1, x2, dp, dbuf, nbuf, hbuf, g0buf, slbuf, drbuf, dmid, tbuf,
           acc_g2, acc_cross, acc_beta, acc_n, acc_f1, acc_f2, gvec, sbuf, gnbuf, qbuf,
           ru, rd, rc, sc, sa, ra, gb, grx, gs, grf, tx, tsum,
           io_sem, hs_sem, hr_sem, as_sem, ar_sem, gs_sem, gr_sem, as2_sem, ar2_sem, ts_sem, tr_sem):
    sw = lax.axis_index('sw')
    sh = lax.axis_index('sh')
    me = sw * QUAD + sh
    other_w = I1 - sw

    def peer(d):
        f = lax.rem(me + d, SUB)
        return {'sw': f // QUAD, 'sh': lax.rem(f, QUAD)}

    barrier = pltpu.get_barrier_semaphore()
    for d in range(I1, SUB):
        pl.semaphore_signal(barrier, inc=I1, device_id=peer(d), device_id_type=MESH)

    def setup():
        spots = ((b_fc1, FC1B), (gamma, GAMMA), (beta, BETA), (b_conv, CONVB),
                 (g_norm, NORMG), (b_norm, NORMB), (b_fc2, FC2B))
        for k in range(PAIR):
            for ref, at in spots:
                n = ref.shape[I1]
                row = jnp.broadcast_to(ref[k:k + I1, :], (LANE, n))
                cols[k, at:at + n, :] = jnp.transpose(row)
            m = jnp.concatenate([mask_in[k:k + I1, :]] * SUB, axis=I1)
            mask[k] = jnp.broadcast_to(m, (SUB, PXL))
            w1t[k] = jnp.transpose(jnp.concatenate([w1[k].astype(F32), jnp.zeros((SUB, HID), F32)], axis=I0)).astype(BF16)
            w2[k] = jnp.transpose(w2t[k].astype(F32)).astype(BF16)
        eb[...] = jnp.zeros_like(eb)
        place = lax.broadcasted_iota(jnp.int32, (PAIR, LANE), I1) // SUB

        def taps_row(i, carry):
            rows = [jnp.concatenate([taps[i, j].astype(F32), jnp.zeros((PAIR, CHQ), F32)], axis=I1) for j in range(TAP)]
            for g in range(NG):
                fwd = jnp.zeros((PAIR, LANE), F32)
                bwd = jnp.zeros((PAIR, LANE), F32)
                for j in range(TAP):
                    fwd = jnp.where(place == j, pltpu.roll(rows[j], (LANE + SUB * (j - g)) % LANE, I1), fwd)
                    bwd = jnp.where(place == TILEH - j, pltpu.roll(rows[j], (LANE + SUB * (TILEH - j - g)) % LANE, I1), bwd)
                eb[I0, g, i, I0:PAIR, :] = fwd
                eb[I1, g, TILEH - i, I0:PAIR, :] = bwd
            return carry
        lax.fori_loop(I0, TAP, taps_row, I0)

    def fetch(src, c):
        return pltpu.make_async_copy(src.at[SUB * c:SUB * c + SUB], io.at[SUB * c:SUB * c + SUB], io_sem.at[c])

    def load_tiles(store):
        unit = jnp.where(lax.broadcasted_iota(jnp.int32, (CH, CH), I0) == lax.broadcasted_iota(jnp.int32, (CH, CH), I1),
                         ONE, ZERO).astype(BF16)

        def step(h, carry):
            for hb in range(PAIR):
                for b in range(IMG):
                    at = hb * 1056 + b * 33
                    xf[at:at + IMG, :] = io[b, hb * TILEH + h].astype(F32)
            for wp in range(QUAD):
                px = []
                for q in range(PAIR):
                    rows = [xf[pl.ds(hb * 1056 + wb * SUB + PAIR * wp + q, IMG, stride=33), :]
                            for hb in range(PAIR) for wb in range(QUAD)]
                    px.append(nt_dot(unit, jnp.concatenate(rows, axis=I0).astype(BF16)))
                for g in range(NG):
                    store(g, h, wp, jnp.concatenate([p[SUB * g:SUB * g + SUB] for p in px], axis=I0).astype(BF16))
            return carry
        lax.fori_loop(I0, TILEH, step, I0)

    def put(dst, h, hb):
        return pltpu.make_async_copy(io.at[:, hb * TILEH + h], dst.at[:, hb * TILEH + h], io_sem.at[h + TILEH * hb])

    def unload_tiles(src, dst):
        def step(h, carry):
            for wp in range(QUAD):
                v = [src[g, QUAD * h + wp].astype(F32) for g in range(NG)]
                for q in range(PAIR):
                    m = jnp.transpose(jnp.concatenate([p[SUB * q:SUB * q + SUB] for p in v], axis=I0))
                    for j in range(SUB):
                        at = (j // QUAD) * 1056 + (j % QUAD) * SUB + PAIR * wp + q
                        xf[pl.ds(at, IMG, stride=33), :] = m[IMG * j:IMG * j + IMG]
            for hb in range(PAIR):
                for b in range(IMG):
                    at = hb * 1056 + b * 33
                    io[b, hb * TILEH + h] = xf[at:at + IMG, :].astype(BF16)
                put(dst, h, hb).start()
            return carry
        lax.fori_loop(I0, TILEH, step, I0)

    def unload_wait(dst):
        for h in range(TILEH):
            for hb in range(PAIR):
                put(dst, h, hb).wait()

    def col(k, off, n, width):
        piece = cols[k, off:off + n, :]
        return jnp.concatenate([piece] * (width // LANE), axis=I1)

    lane128 = lax.broadcasted_iota(jnp.int32, (SUB, LANE), I1)
    grp = lane128 // IMG

    def halo_copies(src, e):
        up = {'sw': sw, 'sh': jnp.maximum(sh - I1, I0)}
        down = {'sw': sw, 'sh': jnp.minimum(sh + I1, RAD)}
        upx = {'sw': other_w, 'sh': jnp.maximum(sh - I1, I0)}
        downx = {'sw': other_w, 'sh': jnp.minimum(sh + I1, RAD)}

        def cp(s, d, i, dev):
            return pltpu.make_async_remote_copy(
                src_ref=s, dst_ref=d, send_sem=hs_sem.at[e, i], recv_sem=hr_sem.at[e, i],
                device_id=dev, device_id_type=MESH)
        return (
            lambda: cp(src.at[:, TILEH:9, PAIR:TILEH, :, LANE:PXL], ru.at[e], I0, down),
            lambda: cp(src.at[:, RAD:TILEH, PAIR:TILEH, :, I0:LANE], rd.at[e], I1, up),
            lambda: cp(sc.at[e], rc.at[e, I1:QUAD], PAIR, {'sw': other_w, 'sh': sh}),
            lambda: cp(sc.at[e, PAIR:RAD], rc.at[e, I0:I1], RAD, downx),
            lambda: cp(sc.at[e, I0:I1], rc.at[e, QUAD:NG], QUAD, upx),
        )

    def halo_start(src, e):
        copies = halo_copies(src, e)

        @pl.when(sh < RAD)
        def _():
            copies[I0]().start()

        @pl.when(sh > I0)
        def _():
            copies[I1]().start()
        first = QUAD - PAIR * sw

        on_left = jnp.where(sw == I0, ONE, ZERO)
        on_right = jnp.where(sw == I1, ONE, ZERO)
        turn = IMG * (I1 - sw)
        for n in range(RAD):
            unit = []
            for a in range(QUAD * n, QUAD * n + QUAD):
                ls = slice((a // TILEH) * LANE, (a // TILEH) * LANE + LANE)
                v = src[:, RAD + a % TILEH, pl.ds(first, PAIR), :, ls].astype(F32).reshape(NG, QUAD, SUB, LANE)
                unit += [v[:, c + I1] * on_left + v[:, c] * on_right for c in range(RAD)]
            pieces = []
            for p in range(RAD):
                out = jnp.zeros((NG, SUB, LANE), F32)
                for q in range(QUAD):
                    out = jnp.where(grp[None] == q, pltpu.roll(unit[QUAD * p + q], lax.rem(q * IMG + turn, LANE), PAIR), out)
                pieces.append(out.reshape(CH, LANE))
            sc[e, n] = jnp.concatenate(pieces, axis=I0).astype(BF16)
        copies[PAIR]().start()

        @pl.when(sh < RAD)
        def _():
            copies[RAD]().start()

        @pl.when(sh > I0)
        def _():
            copies[QUAD]().start()

        @pl.when(sh == I0)
        def _():
            ru[e] = jnp.zeros(ru.shape[I1:], BF16)
            rc[e, I0] = jnp.zeros((120, LANE), BF16)

        @pl.when(sh == RAD)
        def _():
            rd[e] = jnp.zeros(rd.shape[I1:], BF16)
            rc[e, QUAD] = jnp.zeros((120, LANE), BF16)

    def halo_finish(src, e):
        copies = halo_copies(src, e)

        @pl.when(sh < RAD)
        def _():
            copies[I0]().wait_send()
            copies[RAD]().wait_send()
            copies[I1]().wait_recv()
            copies[QUAD]().wait_recv()

        @pl.when(sh > I0)
        def _():
            copies[I1]().wait_send()
            copies[QUAD]().wait_send()
            copies[I0]().wait_recv()
            copies[RAD]().wait_recv()
        copies[PAIR]().wait()
        for r in range(RAD):
            src[:, r, PAIR:TILEH, :, I0:LANE] = ru[e, :, r]
            src[:, 9 + r, PAIR:TILEH, :, LANE:PXL] = rd[e, :, r]
        for r in range(RAD):
            pad_row(src, r, I0)
            pad_row(src, 9 + r, I1)
        spot = lane128 - TQ * (I1 - sw)
        edge_lanes = jnp.logical_and(spot >= I0, spot < IMG)[None]
        side = TILEH - TILEH * sw
        on_left = jnp.where(sw == I0, ONE, ZERO)
        on_right = jnp.where(sw == I1, ONE, ZERO)
        for quad in range(NG):
            strip = rc[e, quad].astype(F32).reshape(RAD, NG, SUB, LANE)
            for rr in range(QUAD):
                spots = [(QUAD * quad + rr - I1 - TILEH * half, half) for half in range(PAIR)]
                spots = [(h, half) for h, half in spots if I0 <= h < PADH]
                edge = []
                for q in range(QUAD if spots else I0):
                    ua, ub = RAD * rr + max(q - I1, I0), RAD * rr + min(q, PAIR)
                    shift = lax.rem(LANE - IMG * (ua % QUAD) + (I1 - sw) * (TQ + IMG * (ua % QUAD - ub % QUAD)), LANE)
                    unit = strip[ua // QUAD]
                    if ua // QUAD != ub // QUAD:
                        unit = unit * on_right + strip[ub // QUAD] * on_left
                    edge.append(pltpu.roll(unit, shift, PAIR))
                for h, half in spots:
                    ls = slice(half * LANE, half * LANE + LANE)
                    old = src[:, h, pl.ds(side, PAIR), :, ls].astype(F32).reshape(NG, QUAD, SUB, LANE)
                    new = [jnp.where(edge_lanes, edge[q], old[:, q])[:, None] for q in range(QUAD)]
                    src[:, h, pl.ds(side, PAIR), :, ls] = jnp.concatenate(new, axis=I1).reshape(NG, PAIR, PR, LANE).astype(BF16)

    def pad_row(src, h, half):
        ls = slice(half * LANE, half * LANE + LANE)
        lanes = lane128[None, None]
        hi = src[:, h, QUAD:TILEH, :, ls].astype(F32).reshape(NG, QUAD, SUB, LANE)
        lo = src[:, h, PAIR:QUAD, :, ls].astype(F32).reshape(NG, QUAD, SUB, LANE)
        left = jnp.where(lanes < IMG, ZERO, pltpu.roll(hi, IMG, RAD))
        right = jnp.where(lanes >= TQ, ZERO, pltpu.roll(lo, TQ, RAD))
        src[:, h, I0:PAIR, :, ls] = left.reshape(NG, PAIR, PR, LANE).astype(BF16)
        src[:, h, TILEH:SUB, :, ls] = right.reshape(NG, PAIR, PR, LANE).astype(BF16)

    def halo_local(src):
        for r in range(RAD):
            src[:, r, PAIR:TILEH, :, LANE:PXL] = src[:, TILEH + r, PAIR:TILEH, :, I0:LANE]
            src[:, 9 + r, PAIR:TILEH, :, I0:LANE] = src[:, RAD + r, PAIR:TILEH, :, LANE:PXL]

        def pad(u, carry):
            pad_row(src, RAD + u, I0)
            pad_row(src, u, I1)
            return carry
        lax.fori_loop(I0, 9, pad, I0, unroll=RAD)

    def fold(ref):
        v = ref[:, I0:LANE] + ref[:, LANE:PXL]
        v = v + pltpu.roll(v, IMG, I1)
        return v + pltpu.roll(v, HALFL, I1)

    def pack_sums(v):
        gq = lax.broadcasted_iota(jnp.int32, (CH, LANE), I1) // IMG
        out = v[I0:CH]
        for q in range(I1, QUAD):
            out = jnp.where(gq == q, v[CH * q:CH * q + CH], out)
        return out

    def unpack_sums(p):
        gq = lax.broadcasted_iota(jnp.int32, (CH, LANE), I1) // IMG
        rows = []
        for q in range(QUAD):
            z = jnp.where(gq == q, p, ZERO)
            z = z + pltpu.roll(z, IMG, I1)
            rows.append(z + pltpu.roll(z, HALFL, I1))
        return jnp.concatenate(rows, axis=I0)

    def reduce_copies(a, n):
        return [pltpu.make_async_remote_copy(
            src_ref=sa.at[a, I0:n], dst_ref=ra.at[a, d - I1, I0:n], send_sem=as_sem.at[a, d - I1], recv_sem=ar_sem.at[a, d - I1],
            device_id=peer(d), device_id_type=MESH) for d in range(I1, SUB)]

    def reduce_start(a, n):
        for c in reduce_copies(a, n):
            c.start()

    def reduce_finish(a, n):
        for c in reduce_copies(a, n):
            c.wait()
        total = sa[a, I0:n]
        for d in range(TAP):
            total = total + ra[a, d, I0:n]
        return total

    def build_band(way, k):
        diag = lax.rem(lax.broadcasted_iota(jnp.int32, (SUB, LANE), I1), SUB) == lax.broadcasted_iota(jnp.int32, (SUB, LANE), I0)

        def one(g, carry):
            base = jnp.concatenate([jnp.where(diag, jnp.broadcast_to(eb[way, g, i, k:k + I1, :], (SUB, LANE)), ZERO)
                                    for i in range(SUB)], axis=I1)
            for h in range(PAIR):
                for wp in range(QUAD):
                    rows = [pltpu.roll(base, h * LANE + (PAIR * wp + q + I1) * SUB, I1) for q in range(PAIR)]
                    at = (h * QUAD + wp) * PR
                    tbuf[g, at:at + PR, :] = jnp.concatenate(rows, axis=I0).astype(BF16)
            return carry
        lax.fori_loop(I0, NG, one, I0, unroll=NG)

    def conv(src, finish):
        def step(hp, carry):
            for g in range(NG):
                tile = src[g, pl.ds(PAIR * hp, SUB)].reshape(BAND, PXL)
                finish(g, hp, dot(tbuf[g], tile))
            return carry
        lax.fori_loop(I0, RAD, step, I0, unroll=RAD)

    def load_pair(ref, i):
        return [ref[g, i].astype(F32).reshape(PAIR, SUB, PXL) for g in range(NG)]

    def to_mat(pieces):
        return jnp.concatenate([jnp.concatenate([p[q] for p in pieces], axis=I0) for q in range(PAIR)], axis=I1)

    def from_mat(m):
        return [jnp.concatenate([m[SUB * g:SUB * g + SUB, I0:PXL][None], m[SUB * g:SUB * g + SUB, PXL:PXP][None]], axis=I0)
                for g in range(NG)]

    def chan_mean(pieces):
        t = pieces[I0]
        for p in pieces[I1:]:
            t = t + p
        return jnp.sum(t, axis=I1, keepdims=True) * (ONE / 40.0)

    def norm_pair(k, i):
        d = [dbuf[k, g, i].astype(F32).reshape(PAIR, SUB, PXL) for g in range(NG)]
        mu = chan_mean(d)
        c = [v - mu for v in d]
        inv = lax.rsqrt(chan_mean([v * v for v in c]) + EPS)
        return [v * inv for v in c], inv

    def gelu_of(x):
        return (0.5 * x) * (ONE + lax.erf(x * 0.7071067811865476))

    def mask_row(k):
        m = mask[k, I0:I1, :]
        return jnp.concatenate([m, m], axis=I1)

    def conv_forward(k, src):
        bias = [col(k, CONVB + SUB * g, SUB, PXL) for g in range(NG)]

        def finish(g, hp, acc):
            v = acc.reshape(PR, SUB, PXL) + bias[g][None]
            dbuf[k, g, pl.ds(SUB * hp, SUB)] = v.reshape(SUB, PR, PXL).astype(BF16)
        conv(src, finish)

    def hidden_forward(k, with_cross):
        acc_g2[...] = jnp.zeros_like(acc_g2)
        if with_cross:
            acc_cross[...] = jnp.zeros_like(acc_cross)

        def step(i, carry):
            nrm, _ = norm_pair(k, i)
            n = [nrm[g] * col(k, NORMG + SUB * g, SUB, PXL)[None] + col(k, NORMB + SUB * g, SUB, PXL)[None] for g in range(NG)]
            n.append(jnp.ones((PAIR, SUB, PXL), F32))
            nb = to_mat(n).astype(BF16)
            nbuf[k, i] = nb
            h = (dot(w1t[k], nb) + col(k, FC1B, HID, PXP)).astype(BF16)
            hbuf[k, i] = h
            g = gelu_of(h.astype(F32))
            if k == I0:
                g0buf[i] = g
            if with_cross:
                cr = drbuf[i].astype(F32) * g
                acc_cross[...] += cr[:, I0:PXL] + cr[:, PXL:PXP]
            g = g * g
            acc_g2[...] += g[:, I0:PXL] + g[:, PXL:PXP]
            return carry
        lax.fori_loop(I0, NPAIR, step, I0, unroll=QUAD)

    def scale_from(k, total):
        gn = jnp.sqrt(unpack_sums(total))
        mean = jnp.sum(gn, axis=I0, keepdims=True) * (ONE / 160.0) + EPS
        gnbuf[k] = gn
        sbuf[k] = cols[k, GAMMA:GAMMA + HID, :] * (gn / mean) + ONE

    def wide(v, width):
        return jnp.concatenate([v] * (width // LANE), axis=I1)

    def resp_of(k, g):
        return (g * wide(sbuf[k], PXP) + col(k, BETA, HID, PXP)).astype(BF16)

    def project(k, i, r, res):
        o = dot(w2t[k], r) + col(k, FC2B, CH, PXP)
        o = from_mat(o * mask_row(k))
        return [(res[g] + o[g]).reshape(PR, PXL).astype(BF16) for g in range(NG)]

    def block1_out():
        def step(i, carry):
            r = resp_of(I0, g0buf[i])
            hh, wp = i // QUAD, lax.rem(i, QUAD)
            res = [x1[g, RAD + hh, PAIR + wp].astype(F32).reshape(PAIR, SUB, PXL) for g in range(NG)]
            y = project(I0, i, r, res)
            for g in range(NG):
                x2[g, RAD + hh, PAIR + wp] = y[g]
            return carry
        lax.fori_loop(I0, NPAIR, step, I0, unroll=QUAD)

    def resp_phase(k, dy, with_cross):
        if with_cross:
            acc_cross[...] = jnp.zeros_like(acc_cross)
        acc_beta[...] = jnp.zeros_like(acc_beta)

        def step(i, carry):
            dm = to_mat(load_pair(dy, i)).astype(BF16)
            dr = (dot(w2[k], dm) * mask_row(k)).astype(BF16)
            drbuf[i] = dr
            dr = dr.astype(F32)
            if with_cross:
                cr = dr * g0buf[i]
                acc_cross[...] += cr[:, I0:PXL] + cr[:, PXL:PXP]
            acc_beta[...] += dr[:, I0:PXL] + dr[:, PXL:PXP]
            return carry
        lax.fori_loop(I0, NPAIR, step, I0, unroll=QUAD)

    def slope_phase(k):
        def step(i, carry):
            x = hbuf[k, i].astype(F32)
            phi = 0.5 + 0.5 * lax.erf(x * 0.7071067811865476)
            slbuf[i] = phi + (x * 0.3989422804014327) * jnp.exp(-0.5 * (x * x))
            return carry
        lax.fori_loop(I0, NPAIR, step, I0, unroll=QUAD)

    def grn_grad(k, total):
        gn = gnbuf[k]
        cross = unpack_sums(total)
        mean = jnp.sum(gn, axis=I0, keepdims=True) * (ONE / 160.0) + EPS
        ds = cols[k, GAMMA:GAMMA + HID, :] * cross
        dg = ds / mean - jnp.sum(ds * gn, axis=I0, keepdims=True) / (mean * mean * 160.0)
        qbuf[...] = dg / gn

    def hidden_backward(k, dy, with_out):
        acc_f1[...] = jnp.zeros_like(acc_f1)
        acc_f2[...] = jnp.zeros_like(acc_f2)
        acc_n[...] = jnp.zeros_like(acc_n)

        def step(i, carry):
            hh, wp = i // QUAD, lax.rem(i, QUAD)
            g = gelu_of(hbuf[k, i].astype(F32)) if k == I1 else g0buf[i]
            r = resp_of(k, g)
            if with_out:
                res = [x2[g_, RAD + hh, PAIR + wp].astype(F32).reshape(PAIR, SUB, PXL) for g_ in range(NG)]
                y = project(k, i, r, res)
                for g_ in range(NG):
                    ytile[g_, i] = y[g_]
            dm = to_mat(load_pair(dy, i))
            dz = jnp.where(mask_row(k) > ZERO, dm, ZERO)
            dz = jnp.concatenate([dz, jnp.zeros((SUB, PXP), F32)], axis=I0).astype(BF16)
            nb = nbuf[k, i]
            rhs = jnp.concatenate([nb, dz], axis=I0)
            dga = drbuf[i].astype(F32) * wide(sbuf[k], PXP) + g * wide(qbuf[...], PXP)
            dh = (dga * slbuf[i]).astype(BF16)
            raug = jnp.concatenate([r, jnp.ones((PR, PXP), BF16)], axis=I0)
            acc_f1[...] += nt_dot(dh, rhs)
            acc_f2[...] += nt_dot(raug, rhs)
            dn = from_mat(dot(w1[k], dh).astype(BF16).astype(F32))
            nrm, inv = norm_pair(k, i)
            dx = [dn[g_] * col(k, NORMG + SUB * g_, SUB, PXL)[None] for g_ in range(NG)]
            m1 = chan_mean(dx)
            m2 = chan_mean([a * b for a, b in zip(dx, nrm)])
            for g_ in range(NG):
                dd = (inv * (dx[g_] - m1 - nrm[g_] * m2)).astype(BF16)
                dp[g_, RAD + hh, PAIR + wp] = dd.reshape(PR, PXL)
                dd = dd.astype(F32)
                pg = dn[g_] * nrm[g_]
                acc_n[I0, SUB * g_:SUB * g_ + SUB, :] += pg[I0] + pg[I1]
                acc_n[I1, SUB * g_:SUB * g_ + SUB, :] += dn[g_][I0] + dn[g_][I1]
                acc_n[PAIR, SUB * g_:SUB * g_ + SUB, :] += dd[I0] + dd[I1]
            return carry
        lax.fori_loop(I0, NPAIR, step, I0, unroll=QUAD)

    def conv_wgrad(k, src):
        sub = lax.broadcasted_iota(jnp.int32, (SUB, BAND), I0)
        lane = lax.rem(lax.broadcasted_iota(jnp.int32, (SUB, BAND), I1), SUB)

        def one(g, carry):
            for hp in range(RAD):
                a = dp[g, RAD + PAIR * hp:NG + PAIR * hp, PAIR:TILEH].reshape(LANE, PXL)
                b = src[g, PAIR * hp:PAIR * hp + SUB].reshape(BAND, PXL)
                part = nt_dot(a, b)
                if hp == I0:
                    gvec[...] = part
                else:
                    gvec[...] += part
            out = jnp.zeros((SUB, BAND), F32)
            for h in range(PAIR):
                for w in range(SUB):
                    at = (h * SUB + w) * SUB
                    out = out + pltpu.roll(gvec[at:at + SUB, :], BAND - (h * LANE + (w + I1) * SUB), I1)
            out = jnp.sum(jnp.where(sub == lane, out, ZERO), axis=I0, keepdims=True)
            rows = jnp.concatenate([out[:, LANE * i:LANE * i + LANE] for i in range(SUB)], axis=I0)
            tx[k, me, pl.ds(SUB * g, SUB), :] = rows
            return carry
        lax.fori_loop(I0, NG, one, I0, unroll=NG)

    def store_grads(k):
        lane = lax.broadcasted_iota(jnp.int32, (HIDP, LANE), I1)
        f1 = jnp.concatenate([acc_f1[...], jnp.zeros((PR, TQ), F32)], axis=I0)
        f1 = jnp.concatenate([f1, jnp.zeros((HIDP, IMG), F32)], axis=I1)
        f2 = jnp.concatenate([acc_f2[...], jnp.zeros((HIDP, IMG), F32)], axis=I1)
        out = jnp.where(lane < CHP, f1, jnp.where(lane < CHQ, f2, ZERO))

        def column(v, lane_at, n):
            c = jnp.sum(v, axis=I1, keepdims=True)
            c = jnp.concatenate([c, jnp.zeros((HIDP - n, I1), F32)], axis=I0)
            return jnp.where(lane == lane_at, c, ZERO)
        gn = gnbuf[k]
        mean = jnp.sum(gn, axis=I0, keepdims=True) * (ONE / 160.0) + EPS
        out = out + column(acc_beta[:, I0:LANE] + acc_beta[:, LANE:PXL], CHQ, HID)
        out = out + column((acc_cross[:, I0:LANE] + acc_cross[:, LANE:PXL]) * (gn / mean), 89, HID)
        for j in range(RAD):
            out = out + column(acc_n[j, :, I0:LANE] + acc_n[j, :, LANE:PXL], 90 + j, CH)
        gb[k, I0:HIDP, :] = out
        gb[k, HIDP:192, :] = jnp.zeros((PR, LANE), F32)

    def conv_backward(dy, out):
        def finish(g, hp, acc):
            v = acc.reshape(SUB, PR, PXL) + dy[g, pl.ds(SUB * hp, SUB)].astype(F32)
            out[g, pl.ds(SUB * hp, SUB)] = v.astype(BF16)
        conv(dp, finish)

    def scatter_copies(k):
        return [pltpu.make_async_remote_copy(
            src_ref=gb.at[k, pl.ds(pl.multiple_of(lax.rem(me + d, SUB) * NPAIR, SUB), NPAIR)], dst_ref=grx.at[k, d - I1],
            send_sem=gs_sem.at[k, d - I1], recv_sem=gr_sem.at[k, d - I1],
            device_id=peer(d), device_id_type=MESH) for d in range(I1, SUB)]

    def gather_copies(k):
        return [pltpu.make_async_remote_copy(
            src_ref=gs.at[k, TAP], dst_ref=gs.at[k, d - I1], send_sem=as2_sem.at[k, d - I1], recv_sem=ar2_sem.at[k, d - I1],
            device_id=peer(d), device_id_type=MESH) for d in range(I1, SUB)]

    def tap_copies(k):
        return [pltpu.make_async_remote_copy(
            src_ref=tx.at[k, me], dst_ref=tx.at[k, me], send_sem=ts_sem.at[k, d - I1], recv_sem=tr_sem.at[k, d - I1],
            device_id=peer(d), device_id_type=MESH) for d in range(I1, SUB)]

    def start_all(copies):
        for c in copies:
            c.start()

    def wait_all(copies):
        for c in copies:
            c.wait()

    def scatter_to_gather(k):
        wait_all(scatter_copies(k))
        mine = gb[k, pl.ds(pl.multiple_of(me * NPAIR, SUB), NPAIR), :]
        for d in range(TAP):
            mine = mine + grx[k, d]
        gs[k, TAP] = mine
        start_all(gather_copies(k))

    def to_x1(g, h, wp, v):
        x1[g, RAD + h, PAIR + wp] = v

    def to_gout(g, h, wp, v):
        gout[g, QUAD * h + wp] = v
    for c in range(QUAD):
        fetch(xin, c).start()
    for c in range(QUAD):
        fetch(xin, c).wait()
    load_tiles(to_x1)
    for c in range(QUAD):
        fetch(gin, c).start()
    pl.semaphore_wait(barrier, TAP)
    halo_start(x1, I0)
    setup()
    build_band(I0, I0)
    halo_local(x1)
    halo_finish(x1, I0)
    conv_forward(I0, x1)
    hidden_forward(I0, False)
    sa[I0, I0:CH] = pack_sums(fold(acc_g2))
    reduce_start(I0, CH)
    for c in range(QUAD):
        fetch(gin, c).wait()
    load_tiles(to_gout)
    build_band(I0, I1)
    total = reduce_finish(I0, CH)
    scale_from(I0, total)
    block1_out()
    halo_start(x2, I1)
    halo_local(x2)
    resp_phase(I1, gout, False)
    halo_finish(x2, I1)
    conv_forward(I1, x2)
    hidden_forward(I1, True)
    sa[I1, I0:CH] = pack_sums(fold(acc_g2))
    sa[I1, CH:80] = pack_sums(fold(acc_cross))
    reduce_start(I1, 80)
    build_band(I1, I1)
    slope_phase(I1)
    total = reduce_finish(I1, 80)
    scale_from(I1, total[I0:CH])
    grn_grad(I1, total[CH:80])
    hidden_backward(I1, gout, True)
    halo_start(dp, PAIR)
    halo_local(dp)
    conv_wgrad(I1, x2)
    store_grads(I1)
    halo_finish(dp, PAIR)
    start_all(scatter_copies(I1))
    start_all(tap_copies(I1))
    conv_backward(gout, dmid)
    resp_phase(I0, dmid, True)
    sa[PAIR, I0:CH] = pack_sums(fold(acc_cross))
    reduce_start(PAIR, CH)
    build_band(I1, I0)
    slope_phase(I0)
    unload_tiles(ytile, act_out)
    total = reduce_finish(PAIR, CH)
    grn_grad(I0, total)
    scatter_to_gather(I1)
    hidden_backward(I0, dmid, False)
    halo_start(dp, RAD)
    store_grads(I0)
    start_all(scatter_copies(I0))
    conv_wgrad(I0, x1)
    start_all(tap_copies(I0))
    halo_local(dp)
    scatter_to_gather(I0)
    halo_finish(dp, RAD)
    conv_backward(dmid, dmid)
    unload_wait(act_out)
    unload_tiles(dmid, grad_in)
    for k in range(PAIR):
        wait_all(tap_copies(k))
        wait_all(gather_copies(k))
        total = tx[k, I0]
        for d in range(I1, SUB):
            total = total + tx[k, d]
        tsum[k] = total
        grf[k, me] = gs[k, TAP]
        for d in range(I1, SUB):
            grf[k, lax.rem(me + SUB - d, SUB)] = gs[k, d - I1]
        gb[k] = grf[k].reshape(192, LANE)
    for k in range(PAIR):
        t = jnp.transpose(gb[k, I0:HID, :])
        o_w1[k] = t[I0:CH]
        o_w2[k] = t[CHP:CHQ] * KEEP
        o_b1[k:k + I1, :] = t[CH:41]
        o_beta[k:k + I1, :] = t[CHQ:89]
        o_gamma[k:k + I1, :] = t[89:90]
        o_gnorm[k:k + I1, :] = t[90:91, I0:CH]
        o_bnorm[k:k + I1, :] = t[91:92, I0:CH]
        o_bconv[k:k + I1, :] = t[92:93, I0:CH]
        o_b2[k:k + I1, :] = gb[k, HID:161, CHP:CHQ] * KEEP
    place = lax.broadcasted_iota(jnp.int32, (PAIR, LANE), I1) // SUB

    def taps_row(i, carry):
        for j in range(TAP):
            out = jnp.zeros((PAIR, LANE), F32)
            for g in range(NG):
                rows = jnp.concatenate([tsum[k, pl.ds(SUB * g + i, I1), :] for k in range(PAIR)], axis=I0)
                out = jnp.where(place == g, pltpu.roll(rows, (LANE + SUB * (g - j)) % LANE, I1), out)
            o_taps[i, j] = out[:, I0:CH]
        return carry
    lax.fori_loop(I0, TAP, taps_row, I0)
    unload_wait(grad_in)


def run_kernel(args):
    vm = pl.BlockSpec(memory_space=pltpu.VMEM)
    hbm = pl.BlockSpec(memory_space=pl.ANY)
    pad = pltpu.VMEM((NG, PADH, SUB, PR, PXL), BF16)
    tiles = pltpu.VMEM((NG, NPAIR, PR, PXL), BF16)
    return pl.pallas_call(
        kernel,
        name='blocks',
        out_shape=out_shapes(),
        in_specs=[hbm] * PAIR + [vm] * (len(args) - PAIR),
        out_specs=(hbm,) * PAIR + (vm,) * 10,
        scratch_shapes=[
            pltpu.VMEM((IMG, PADH, IMG, CH), BF16), pltpu.VMEM((2112, CH), F32), tiles, tiles,
            pltpu.VMEM((PAIR, SUB, PXL), F32), pltpu.VMEM((PAIR, NG, SUB, SUB, LANE), F32), pltpu.VMEM((PAIR, 640, LANE), F32),
            pltpu.VMEM((PAIR, HID, CHP), BF16), pltpu.VMEM((PAIR, HID, CH), BF16),
            pad, pad, pad,
            pltpu.VMEM((PAIR, NG, NPAIR, PR, PXL), BF16),
            pltpu.VMEM((PAIR, NPAIR, CHP, PXP), BF16),
            pltpu.VMEM((PAIR, NPAIR, HID, PXP), BF16),
            pltpu.VMEM((NPAIR, HID, PXP), F32), pltpu.VMEM((NPAIR, HID, PXP), F32),
            pltpu.VMEM((NPAIR, HID, PXP), BF16),
            pltpu.VMEM((NG, NPAIR, PR, PXL), BF16),
            pltpu.VMEM((NG, LANE, BAND), BF16),
            pltpu.VMEM((HID, PXL), F32), pltpu.VMEM((HID, PXL), F32), pltpu.VMEM((HID, PXL), F32),
            pltpu.VMEM((RAD, CH, PXL), F32),
            pltpu.VMEM((HID, TQ), F32), pltpu.VMEM((HIDP, TQ), F32),
            pltpu.VMEM((LANE, BAND), F32),
            pltpu.VMEM((PAIR, HID, LANE), F32), pltpu.VMEM((PAIR, HID, LANE), F32), pltpu.VMEM((HID, LANE), F32),
            pltpu.VMEM((QUAD, NG, RAD, QUAD, PR, LANE), BF16), pltpu.VMEM((QUAD, NG, RAD, QUAD, PR, LANE), BF16),
            pltpu.VMEM((QUAD, NG, 120, LANE), BF16), pltpu.VMEM((QUAD, RAD, 120, LANE), BF16),
            pltpu.VMEM((RAD, 80, LANE), F32), pltpu.VMEM((RAD, TAP, 80, LANE), F32),
            pltpu.VMEM((PAIR, 192, LANE), F32), pltpu.VMEM((PAIR, TAP, NPAIR, LANE), F32), pltpu.VMEM((PAIR, SUB, NPAIR, LANE), F32),
            pltpu.VMEM((PAIR, SUB, NPAIR, LANE), F32), pltpu.VMEM((PAIR, SUB, CH, LANE), F32), pltpu.VMEM((PAIR, CH, LANE), F32),
            pltpu.SemaphoreType.DMA((PADH,)),
            pltpu.SemaphoreType.DMA((QUAD, NG)), pltpu.SemaphoreType.DMA((QUAD, NG)),
            pltpu.SemaphoreType.DMA((RAD, TAP)), pltpu.SemaphoreType.DMA((RAD, TAP)),
        ] + [pltpu.SemaphoreType.DMA((PAIR, TAP))] * TILEH,
        compiler_params=pltpu.CompilerParams(collective_id=I0, has_side_effects=True, vmem_limit_bytes=67043328),
    )(*args)


def out_shapes():
    shape = lambda *d: jax.ShapeDtypeStruct(d, F32)
    act = jax.ShapeDtypeStruct((IMG, PADH, IMG, CH), BF16)
    small, wide = shape(PAIR, CH), shape(PAIR, HID)
    return (act, act, shape(TAP, TAP, PAIR, CH), small, small, small, shape(PAIR, CH, HID), wide, wide, wide, shape(PAIR, CH, HID), small)


def finish_kernel(*refs):
    n = len(refs) // RAD
    src, dst, mid = refs[I0:n], refs[n:PAIR * n], refs[PAIR * n:RAD * n]
    in_sem, out_sem = refs[RAD * n:]
    moves = []
    for a in range(n):
        cuts = [slice(SUB * c, SUB * c + SUB) for c in range(QUAD)] if a < PAIR else [slice(None)]
        for cut in cuts:
            moves.append((src[a].at[cut], mid[a].at[cut], dst[a].at[cut]))
    ins = [pltpu.make_async_copy(m[I0], m[I1], in_sem.at[c]) for c, m in enumerate(moves)]
    outs = [pltpu.make_async_copy(m[I1], m[PAIR], out_sem.at[c]) for c, m in enumerate(moves)]
    for c in ins:
        c.start()
    for c, o in zip(ins, outs):
        c.wait()
        o.start()
    for o in outs:
        o.wait()


def finish(parts):
    n = len(parts)
    hbm = pl.BlockSpec(memory_space=pl.ANY)
    return pl.pallas_call(
        finish_kernel, name='finish', out_shape=out_shapes(),
        in_specs=[hbm] * n, out_specs=(hbm,) * n,
        scratch_shapes=[pltpu.VMEM(o.shape, o.dtype) for o in out_shapes()] + [pltpu.SemaphoreType.DMA((n + TILEH,))] * PAIR,
        compiler_params=pltpu.CompilerParams(vmem_limit_bytes=67043328),
    )(*parts)


def solution(mesh):
    act_spec = P('dp', 'sh', 'sw', None)
    rep = P()

    def local_step(act_in, drop_mask, grad_out, conv_w, conv_b, norm_g, norm_b, fc1_w, fc1_b, grn_gamma, grn_beta, fc2_w, fc2_b):
        parts = run_kernel((act_in, grad_out, drop_mask.T, conv_w.transpose(I1, PAIR, I0, RAD), fc1_b, grn_gamma, grn_beta,
                            conv_b, norm_g, norm_b, fc2_b, fc1_w, fc2_w.transpose(I0, PAIR, I1)))
        act_out, grad_in, taps, *rest = finish(parts)
        rest[TAP] = rest[TAP].transpose(I0, PAIR, I1)
        return (act_out, grad_in, taps.transpose(PAIR, I0, I1, RAD), *rest)

    return jax.shard_map(local_step, mesh=mesh,
                         in_specs=(act_spec, P('dp', None), act_spec) + (rep,) * 10,
                         out_specs=(act_spec, act_spec) + (P('dp'),) * 10,
                         check_vma=False)
```

```python
import functools

import jax
import jax.numpy as jnp
import numpy as np
from jax import lax
from jax.experimental import pallas as pl
from jax.experimental.pallas import tpu as pltpu
from jax.sharding import PartitionSpec as P

EPS = 1e-6
F32 = jnp.float32
BF16 = jnp.bfloat16
MESH = pl.DeviceIdType.MESH
NG = 5
NPAIR = 24
ROWS = 224
KEEP = 4.0 / 3.0
FC1B, GAMMA, BETA, CONVB, NORMG, NORMB, FC2B = 0, 160, 320, 480, 520, 560, 600


LANE = 128
PXL = 256
PXP = 512
SUB = 8
CH = 40
HID = 160
IMG = 32
PR = 16
TQ = 96
CHP = 48
BAND = 1024
HIDP = 176
CHQ = 88
HALFL = 64
PADH = 12
ZERO = 0.0
ONE = 1.0
TAP = 7
TILEH = 6
QUAD = 4
RAD = 3
PAIR = 2
I0 = 0
I1 = 1


def nt_dot(a, b):
    return lax.dot_general(a, b, (((I1,), (I1,)), ((), ())), preferred_element_type=F32)


def dot(a, b):
    return jnp.dot(a, b, preferred_element_type=F32)


def kernel(xin, gin, mask_in, taps, b_fc1, gamma, beta, b_conv, g_norm, b_norm, b_fc2, w1, w2t,
           act_out, grad_in, o_taps, o_bconv, o_gnorm, o_bnorm, o_w1, o_b1, o_gamma, o_beta, o_w2, o_b2,
           io, xf, gout, ytile, mask, eb, cols, w1t, w2, x1, x2, dp, dbuf, nbuf, hbuf, g0buf, slbuf, drbuf, dmid, tbuf,
           acc_g2, acc_cross, acc_beta, acc_n, acc_f1, acc_f2, gvec, sbuf, gnbuf, qbuf,
           ru, rd, rc, sc, sa, ra, gb, grx, gs, grf, tx, tsum,
           io_sem, hs_sem, hr_sem, as_sem, ar_sem, gs_sem, gr_sem, as2_sem, ar2_sem, ts_sem, tr_sem):
    sw = lax.axis_index('sw')
    sh = lax.axis_index('sh')
    me = sw * QUAD + sh
    other_w = I1 - sw

    def peer(d):
        f = lax.rem(me + d, SUB)
        return {'sw': f // QUAD, 'sh': lax.rem(f, QUAD)}

    barrier = pltpu.get_barrier_semaphore()
    for d in range(I1, SUB):
        pl.semaphore_signal(barrier, inc=I1, device_id=peer(d), device_id_type=MESH)

    def setup():
        spots = ((b_fc1, FC1B), (gamma, GAMMA), (beta, BETA), (b_conv, CONVB),
                 (g_norm, NORMG), (b_norm, NORMB), (b_fc2, FC2B))
        for k in range(PAIR):
            for ref, at in spots:
                n = ref.shape[I1]
                row = jnp.broadcast_to(ref[k:k + I1, :], (LANE, n))
                cols[k, at:at + n, :] = jnp.transpose(row)
            m = jnp.concatenate([mask_in[k:k + I1, :]] * SUB, axis=I1)
            mask[k] = jnp.broadcast_to(m, (SUB, PXL))
            w1t[k] = jnp.transpose(jnp.concatenate([w1[k].astype(F32), jnp.zeros((SUB, HID), F32)], axis=I0)).astype(BF16)
            w2[k] = jnp.transpose(w2t[k].astype(F32)).astype(BF16)
        eb[...] = jnp.zeros_like(eb)
        place = lax.broadcasted_iota(jnp.int32, (PAIR, LANE), I1) // SUB

        def taps_row(i, carry):
            rows = [jnp.concatenate([taps[i, j].astype(F32), jnp.zeros((PAIR, CHQ), F32)], axis=I1) for j in range(TAP)]
            for g in range(NG):
                fwd = jnp.zeros((PAIR, LANE), F32)
                bwd = jnp.zeros((PAIR, LANE), F32)
                for j in range(TAP):
                    fwd = jnp.where(place == j, pltpu.roll(rows[j], (LANE + SUB * (j - g)) % LANE, I1), fwd)
                    bwd = jnp.where(place == TILEH - j, pltpu.roll(rows[j], (LANE + SUB * (TILEH - j - g)) % LANE, I1), bwd)
                eb[I0, g, i, I0:PAIR, :] = fwd
                eb[I1, g, TILEH - i, I0:PAIR, :] = bwd
            return carry
        lax.fori_loop(I0, TAP, taps_row, I0)

    def fetch(src, c):
        return pltpu.make_async_copy(src.at[SUB * c:SUB * c + SUB], io.at[SUB * c:SUB * c + SUB], io_sem.at[c])

    def load_tiles(store):
        unit = jnp.where(lax.broadcasted_iota(jnp.int32, (CH, CH), I0) == lax.broadcasted_iota(jnp.int32, (CH, CH), I1),
                         ONE, ZERO).astype(BF16)

        def step(h, carry):
            for hb in range(PAIR):
                for b in range(IMG):
                    at = hb * 1056 + b * 33
                    xf[at:at + IMG, :] = io[b, hb * TILEH + h].astype(F32)
            for wp in range(QUAD):
                px = []
                for q in range(PAIR):
                    rows = [xf[pl.ds(hb * 1056 + wb * SUB + PAIR * wp + q, IMG, stride=33), :]
                            for hb in range(PAIR) for wb in range(QUAD)]
                    px.append(nt_dot(unit, jnp.concatenate(rows, axis=I0).astype(BF16)))
                for g in range(NG):
                    store(g, h, wp, jnp.concatenate([p[SUB * g:SUB * g + SUB] for p in px], axis=I0).astype(BF16))
            return carry
        lax.fori_loop(I0, TILEH, step, I0)

    def put(dst, h, hb):
        return pltpu.make_async_copy(io.at[:, hb * TILEH + h], dst.at[:, hb * TILEH + h], io_sem.at[h + TILEH * hb])

    def unload_tiles(src, dst):
        def step(h, carry):
            for wp in range(QUAD):
                v = [src[g, QUAD * h + wp].astype(F32) for g in range(NG)]
                for q in range(PAIR):
                    m = jnp.transpose(jnp.concatenate([p[SUB * q:SUB * q + SUB] for p in v], axis=I0))
                    for j in range(SUB):
                        at = (j // QUAD) * 1056 + (j % QUAD) * SUB + PAIR * wp + q
                        xf[pl.ds(at, IMG, stride=33), :] = m[IMG * j:IMG * j + IMG]
            for hb in range(PAIR):
                for b in range(IMG):
                    at = hb * 1056 + b * 33
                    io[b, hb * TILEH + h] = xf[at:at + IMG, :].astype(BF16)
                put(dst, h, hb).start()
            return carry
        lax.fori_loop(I0, TILEH, step, I0, unroll=PAIR)

    def unload_wait(dst):
        for h in range(TILEH):
            for hb in range(PAIR):
                put(dst, h, hb).wait()

    def col(k, off, n, width):
        piece = cols[k, off:off + n, :]
        return jnp.concatenate([piece] * (width // LANE), axis=I1)

    lane128 = lax.broadcasted_iota(jnp.int32, (SUB, LANE), I1)
    grp = lane128 // IMG

    def halo_copies(src, e):
        up = {'sw': sw, 'sh': jnp.maximum(sh - I1, I0)}
        down = {'sw': sw, 'sh': jnp.minimum(sh + I1, RAD)}
        upx = {'sw': other_w, 'sh': jnp.maximum(sh - I1, I0)}
        downx = {'sw': other_w, 'sh': jnp.minimum(sh + I1, RAD)}

        def cp(s, d, i, dev):
            return pltpu.make_async_remote_copy(
                src_ref=s, dst_ref=d, send_sem=hs_sem.at[e, i], recv_sem=hr_sem.at[e, i],
                device_id=dev, device_id_type=MESH)
        return (
            lambda: cp(src.at[:, TILEH:9, PAIR:TILEH, :, LANE:PXL], ru.at[e], I0, down),
            lambda: cp(src.at[:, RAD:TILEH, PAIR:TILEH, :, I0:LANE], rd.at[e], I1, up),
            lambda: cp(sc.at[e], rc.at[e, I1:QUAD], PAIR, {'sw': other_w, 'sh': sh}),
            lambda: cp(sc.at[e, PAIR:RAD], rc.at[e, I0:I1], RAD, downx),
            lambda: cp(sc.at[e, I0:I1], rc.at[e, QUAD:NG], QUAD, upx),
        )

    def halo_start(src, e):
        copies = halo_copies(src, e)

        @pl.when(sh < RAD)
        def _():
            copies[I0]().start()

        @pl.when(sh > I0)
        def _():
            copies[I1]().start()
        first = QUAD - PAIR * sw

        on_left = jnp.where(sw == I0, ONE, ZERO)
        on_right = jnp.where(sw == I1, ONE, ZERO)
        turn = IMG * (I1 - sw)
        for n in range(RAD):
            unit = []
            for a in range(QUAD * n, QUAD * n + QUAD):
                ls = slice((a // TILEH) * LANE, (a // TILEH) * LANE + LANE)
                v = src[:, RAD + a % TILEH, pl.ds(first, PAIR), :, ls].astype(F32).reshape(NG, QUAD, SUB, LANE)
                unit += [v[:, c + I1] * on_left + v[:, c] * on_right for c in range(RAD)]
            pieces = []
            for p in range(RAD):
                out = jnp.zeros((NG, SUB, LANE), F32)
                for q in range(QUAD):
                    out = jnp.where(grp[None] == q, pltpu.roll(unit[QUAD * p + q], lax.rem(q * IMG + turn, LANE), PAIR), out)
                pieces.append(out.reshape(CH, LANE))
            sc[e, n] = jnp.concatenate(pieces, axis=I0).astype(BF16)
        copies[PAIR]().start()

        @pl.when(sh < RAD)
        def _():
            copies[RAD]().start()

        @pl.when(sh > I0)
        def _():
            copies[QUAD]().start()

        @pl.when(sh == I0)
        def _():
            ru[e] = jnp.zeros(ru.shape[I1:], BF16)
            rc[e, I0] = jnp.zeros((120, LANE), BF16)

        @pl.when(sh == RAD)
        def _():
            rd[e] = jnp.zeros(rd.shape[I1:], BF16)
            rc[e, QUAD] = jnp.zeros((120, LANE), BF16)

    def halo_finish(src, e):
        copies = halo_copies(src, e)

        @pl.when(sh < RAD)
        def _():
            copies[I0]().wait_send()
            copies[RAD]().wait_send()
            copies[I1]().wait_recv()
            copies[QUAD]().wait_recv()

        @pl.when(sh > I0)
        def _():
            copies[I1]().wait_send()
            copies[QUAD]().wait_send()
            copies[I0]().wait_recv()
            copies[RAD]().wait_recv()
        copies[PAIR]().wait()
        for r in range(RAD):
            src[:, r, PAIR:TILEH, :, I0:LANE] = ru[e, :, r]
            src[:, 9 + r, PAIR:TILEH, :, LANE:PXL] = rd[e, :, r]
        for r in range(RAD):
            pad_row(src, r, I0)
            pad_row(src, 9 + r, I1)
        spot = lane128 - TQ * (I1 - sw)
        edge_lanes = jnp.logical_and(spot >= I0, spot < IMG)[None]
        side = TILEH - TILEH * sw
        on_left = jnp.where(sw == I0, ONE, ZERO)
        on_right = jnp.where(sw == I1, ONE, ZERO)
        for quad in range(NG):
            strip = rc[e, quad].astype(F32).reshape(RAD, NG, SUB, LANE)
            for rr in range(QUAD):
                spots = [(QUAD * quad + rr - I1 - TILEH * half, half) for half in range(PAIR)]
                spots = [(h, half) for h, half in spots if I0 <= h < PADH]
                edge = []
                for q in range(QUAD if spots else I0):
                    ua, ub = RAD * rr + max(q - I1, I0), RAD * rr + min(q, PAIR)
                    shift = lax.rem(LANE - IMG * (ua % QUAD) + (I1 - sw) * (TQ + IMG * (ua % QUAD - ub % QUAD)), LANE)
                    unit = strip[ua // QUAD]
                    if ua // QUAD != ub // QUAD:
                        unit = unit * on_right + strip[ub // QUAD] * on_left
                    edge.append(pltpu.roll(unit, shift, PAIR))
                for h, half in spots:
                    ls = slice(half * LANE, half * LANE + LANE)
                    old = src[:, h, pl.ds(side, PAIR), :, ls].astype(F32).reshape(NG, QUAD, SUB, LANE)
                    new = [jnp.where(edge_lanes, edge[q], old[:, q])[:, None] for q in range(QUAD)]
                    src[:, h, pl.ds(side, PAIR), :, ls] = jnp.concatenate(new, axis=I1).reshape(NG, PAIR, PR, LANE).astype(BF16)

    def pad_row(src, h, half):
        ls = slice(half * LANE, half * LANE + LANE)
        lanes = lane128[None, None]
        hi = src[:, h, QUAD:TILEH, :, ls].astype(F32).reshape(NG, QUAD, SUB, LANE)
        lo = src[:, h, PAIR:QUAD, :, ls].astype(F32).reshape(NG, QUAD, SUB, LANE)
        left = jnp.where(lanes < IMG, ZERO, pltpu.roll(hi, IMG, RAD))
        right = jnp.where(lanes >= TQ, ZERO, pltpu.roll(lo, TQ, RAD))
        src[:, h, I0:PAIR, :, ls] = left.reshape(NG, PAIR, PR, LANE).astype(BF16)
        src[:, h, TILEH:SUB, :, ls] = right.reshape(NG, PAIR, PR, LANE).astype(BF16)

    def halo_local(src):
        for r in range(RAD):
            src[:, r, PAIR:TILEH, :, LANE:PXL] = src[:, TILEH + r, PAIR:TILEH, :, I0:LANE]
            src[:, 9 + r, PAIR:TILEH, :, I0:LANE] = src[:, RAD + r, PAIR:TILEH, :, LANE:PXL]

        def pad(u, carry):
            pad_row(src, RAD + u, I0)
            pad_row(src, u, I1)
            return carry
        lax.fori_loop(I0, 9, pad, I0, unroll=9)

    def fold(ref):
        v = ref[:, I0:LANE] + ref[:, LANE:PXL]
        v = v + pltpu.roll(v, IMG, I1)
        return v + pltpu.roll(v, HALFL, I1)

    def pack_sums(v):
        gq = lax.broadcasted_iota(jnp.int32, (CH, LANE), I1) // IMG
        out = v[I0:CH]
        for q in range(I1, QUAD):
            out = jnp.where(gq == q, v[CH * q:CH * q + CH], out)
        return out

    def unpack_sums(p):
        gq = lax.broadcasted_iota(jnp.int32, (CH, LANE), I1) // IMG
        rows = []
        for q in range(QUAD):
            z = jnp.where(gq == q, p, ZERO)
            z = z + pltpu.roll(z, IMG, I1)
            rows.append(z + pltpu.roll(z, HALFL, I1))
        return jnp.concatenate(rows, axis=I0)

    def reduce_copies(a, n):
        return [pltpu.make_async_remote_copy(
            src_ref=sa.at[a, I0:n], dst_ref=ra.at[a, d - I1, I0:n], send_sem=as_sem.at[a, d - I1], recv_sem=ar_sem.at[a, d - I1],
            device_id=peer(d), device_id_type=MESH) for d in range(I1, SUB)]

    def reduce_start(a, n):
        for c in reduce_copies(a, n):
            c.start()

    def reduce_finish(a, n):
        for c in reduce_copies(a, n):
            c.wait()
        total = sa[a, I0:n]
        for d in range(TAP):
            total = total + ra[a, d, I0:n]
        return total

    def build_band(way, k):
        diag = lax.rem(lax.broadcasted_iota(jnp.int32, (SUB, LANE), I1), SUB) == lax.broadcasted_iota(jnp.int32, (SUB, LANE), I0)

        def one(g, carry):
            base = jnp.concatenate([jnp.where(diag, jnp.broadcast_to(eb[way, g, i, k:k + I1, :], (SUB, LANE)), ZERO)
                                    for i in range(SUB)], axis=I1)
            for h in range(PAIR):
                for wp in range(QUAD):
                    rows = [pltpu.roll(base, h * LANE + (PAIR * wp + q + I1) * SUB, I1) for q in range(PAIR)]
                    at = (h * QUAD + wp) * PR
                    tbuf[g, at:at + PR, :] = jnp.concatenate(rows, axis=I0).astype(BF16)
            return carry
        lax.fori_loop(I0, NG, one, I0, unroll=NG)

    def conv(src, finish):
        def step(hp, carry):
            for g in range(NG):
                tile = src[g, pl.ds(PAIR * hp, SUB)].reshape(BAND, PXL)
                finish(g, hp, dot(tbuf[g], tile))
            return carry
        lax.fori_loop(I0, RAD, step, I0, unroll=RAD)

    def load_pair(ref, i):
        return [ref[g, i].astype(F32).reshape(PAIR, SUB, PXL) for g in range(NG)]

    def to_mat(pieces):
        return jnp.concatenate([jnp.concatenate([p[q] for p in pieces], axis=I0) for q in range(PAIR)], axis=I1)

    def from_mat(m):
        return [jnp.concatenate([m[SUB * g:SUB * g + SUB, I0:PXL][None], m[SUB * g:SUB * g + SUB, PXL:PXP][None]], axis=I0)
                for g in range(NG)]

    def chan_mean(pieces):
        t = pieces[I0]
        for p in pieces[I1:]:
            t = t + p
        return jnp.sum(t, axis=I1, keepdims=True) * (ONE / 40.0)

    def norm_pair(k, i):
        d = [dbuf[k, g, i].astype(F32).reshape(PAIR, SUB, PXL) for g in range(NG)]
        mu = chan_mean(d)
        c = [v - mu for v in d]
        inv = lax.rsqrt(chan_mean([v * v for v in c]) + EPS)
        return [v * inv for v in c], inv

    def gelu_of(x):
        return (0.5 * x) * (ONE + lax.erf(x * 0.7071067811865476))

    def mask_row(k):
        m = mask[k, I0:I1, :]
        return jnp.concatenate([m, m], axis=I1)

    def conv_forward(k, src):
        bias = [col(k, CONVB + SUB * g, SUB, PXL) for g in range(NG)]

        def finish(g, hp, acc):
            v = acc.reshape(PR, SUB, PXL) + bias[g][None]
            dbuf[k, g, pl.ds(SUB * hp, SUB)] = v.reshape(SUB, PR, PXL).astype(BF16)
        conv(src, finish)

    def hidden_forward(k, with_cross):
        acc_g2[...] = jnp.zeros_like(acc_g2)
        if with_cross:
            acc_cross[...] = jnp.zeros_like(acc_cross)

        def step(i, carry):
            nrm, _ = norm_pair(k, i)
            n = [nrm[g] * col(k, NORMG + SUB * g, SUB, PXL)[None] + col(k, NORMB + SUB * g, SUB, PXL)[None] for g in range(NG)]
            n.append(jnp.ones((PAIR, SUB, PXL), F32))
            nb = to_mat(n).astype(BF16)
            nbuf[k, i] = nb
            h = (dot(w1t[k], nb) + col(k, FC1B, HID, PXP)).astype(BF16)
            hbuf[k, i] = h
            g = gelu_of(h.astype(F32))
            if k == I0:
                g0buf[i] = g
            if with_cross:
                cr = drbuf[i].astype(F32) * g
                acc_cross[...] += cr[:, I0:PXL] + cr[:, PXL:PXP]
            g = g * g
            acc_g2[...] += g[:, I0:PXL] + g[:, PXL:PXP]
            return carry
        lax.fori_loop(I0, NPAIR, step, I0, unroll=QUAD)

    def scale_from(k, total):
        gn = jnp.sqrt(unpack_sums(total))
        mean = jnp.sum(gn, axis=I0, keepdims=True) * (ONE / 160.0) + EPS
        gnbuf[k] = gn
        sbuf[k] = cols[k, GAMMA:GAMMA + HID, :] * (gn / mean) + ONE

    def wide(v, width):
        return jnp.concatenate([v] * (width // LANE), axis=I1)

    def resp_of(k, g):
        return (g * wide(sbuf[k], PXP) + col(k, BETA, HID, PXP)).astype(BF16)

    def project(k, i, r, res):
        o = dot(w2t[k], r) + col(k, FC2B, CH, PXP)
        o = from_mat(o * mask_row(k))
        return [(res[g] + o[g]).reshape(PR, PXL).astype(BF16) for g in range(NG)]

    def block1_out():
        def step(i, carry):
            r = resp_of(I0, g0buf[i])
            hh, wp = i // QUAD, lax.rem(i, QUAD)
            res = [x1[g, RAD + hh, PAIR + wp].astype(F32).reshape(PAIR, SUB, PXL) for g in range(NG)]
            y = project(I0, i, r, res)
            for g in range(NG):
                x2[g, RAD + hh, PAIR + wp] = y[g]
            return carry
        lax.fori_loop(I0, NPAIR, step, I0, unroll=QUAD)

    def resp_phase(k, dy, with_cross):
        if with_cross:
            acc_cross[...] = jnp.zeros_like(acc_cross)
        acc_beta[...] = jnp.zeros_like(acc_beta)

        def step(i, carry):
            dm = to_mat(load_pair(dy, i)).astype(BF16)
            dr = (dot(w2[k], dm) * mask_row(k)).astype(BF16)
            drbuf[i] = dr
            dr = dr.astype(F32)
            if with_cross:
                cr = dr * g0buf[i]
                acc_cross[...] += cr[:, I0:PXL] + cr[:, PXL:PXP]
            acc_beta[...] += dr[:, I0:PXL] + dr[:, PXL:PXP]
            return carry
        lax.fori_loop(I0, NPAIR, step, I0, unroll=QUAD)

    def slope_phase(k):
        def step(i, carry):
            x = hbuf[k, i].astype(F32)
            phi = 0.5 + 0.5 * lax.erf(x * 0.7071067811865476)
            slbuf[i] = phi + (x * 0.3989422804014327) * jnp.exp(-0.5 * (x * x))
            return carry
        lax.fori_loop(I0, NPAIR, step, I0, unroll=QUAD)

    def grn_grad(k, total):
        gn = gnbuf[k]
        cross = unpack_sums(total)
        mean = jnp.sum(gn, axis=I0, keepdims=True) * (ONE / 160.0) + EPS
        ds = cols[k, GAMMA:GAMMA + HID, :] * cross
        dg = ds / mean - jnp.sum(ds * gn, axis=I0, keepdims=True) / (mean * mean * 160.0)
        qbuf[...] = dg / gn

    def hidden_backward(k, dy, with_out):
        acc_f1[...] = jnp.zeros_like(acc_f1)
        acc_f2[...] = jnp.zeros_like(acc_f2)
        acc_n[...] = jnp.zeros_like(acc_n)

        def step(i, carry):
            hh, wp = i // QUAD, lax.rem(i, QUAD)
            g = gelu_of(hbuf[k, i].astype(F32)) if k == I1 else g0buf[i]
            r = resp_of(k, g)
            if with_out:
                res = [x2[g_, RAD + hh, PAIR + wp].astype(F32).reshape(PAIR, SUB, PXL) for g_ in range(NG)]
                y = project(k, i, r, res)
                for g_ in range(NG):
                    ytile[g_, i] = y[g_]
            dm = to_mat(load_pair(dy, i))
            dz = jnp.where(mask_row(k) > ZERO, dm, ZERO)
            dz = jnp.concatenate([dz, jnp.zeros((SUB, PXP), F32)], axis=I0).astype(BF16)
            nb = nbuf[k, i]
            rhs = jnp.concatenate([nb, dz], axis=I0)
            dga = drbuf[i].astype(F32) * wide(sbuf[k], PXP) + g * wide(qbuf[...], PXP)
            dh = (dga * slbuf[i]).astype(BF16)
            raug = jnp.concatenate([r, jnp.ones((PR, PXP), BF16)], axis=I0)
            acc_f1[...] += nt_dot(dh, rhs)
            acc_f2[...] += nt_dot(raug, rhs)
            dn = from_mat(dot(w1[k], dh).astype(BF16).astype(F32))
            nrm, inv = norm_pair(k, i)
            dx = [dn[g_] * col(k, NORMG + SUB * g_, SUB, PXL)[None] for g_ in range(NG)]
            m1 = chan_mean(dx)
            m2 = chan_mean([a * b for a, b in zip(dx, nrm)])
            for g_ in range(NG):
                dd = (inv * (dx[g_] - m1 - nrm[g_] * m2)).astype(BF16)
                dp[g_, RAD + hh, PAIR + wp] = dd.reshape(PR, PXL)
                dd = dd.astype(F32)
                pg = dn[g_] * nrm[g_]
                acc_n[I0, SUB * g_:SUB * g_ + SUB, :] += pg[I0] + pg[I1]
                acc_n[I1, SUB * g_:SUB * g_ + SUB, :] += dn[g_][I0] + dn[g_][I1]
                acc_n[PAIR, SUB * g_:SUB * g_ + SUB, :] += dd[I0] + dd[I1]
            return carry
        lax.fori_loop(I0, NPAIR, step, I0, unroll=QUAD)

    def conv_wgrad(k, src):
        sub = lax.broadcasted_iota(jnp.int32, (SUB, BAND), I0)
        lane = lax.rem(lax.broadcasted_iota(jnp.int32, (SUB, BAND), I1), SUB)

        def one(g, carry):
            for hp in range(RAD):
                a = dp[g, RAD + PAIR * hp:NG + PAIR * hp, PAIR:TILEH].reshape(LANE, PXL)
                b = src[g, PAIR * hp:PAIR * hp + SUB].reshape(BAND, PXL)
                part = nt_dot(a, b)
                if hp == I0:
                    gvec[...] = part
                else:
                    gvec[...] += part
            out = jnp.zeros((SUB, BAND), F32)
            for h in range(PAIR):
                for w in range(SUB):
                    at = (h * SUB + w) * SUB
                    out = out + pltpu.roll(gvec[at:at + SUB, :], BAND - (h * LANE + (w + I1) * SUB), I1)
            out = jnp.sum(jnp.where(sub == lane, out, ZERO), axis=I0, keepdims=True)
            rows = jnp.concatenate([out[:, LANE * i:LANE * i + LANE] for i in range(SUB)], axis=I0)
            tx[k, me, pl.ds(SUB * g, SUB), :] = rows
            return carry
        lax.fori_loop(I0, NG, one, I0, unroll=NG)

    def store_grads(k):
        lane = lax.broadcasted_iota(jnp.int32, (HIDP, LANE), I1)
        f1 = jnp.concatenate([acc_f1[...], jnp.zeros((PR, TQ), F32)], axis=I0)
        f1 = jnp.concatenate([f1, jnp.zeros((HIDP, IMG), F32)], axis=I1)
        f2 = jnp.concatenate([acc_f2[...], jnp.zeros((HIDP, IMG), F32)], axis=I1)
        out = jnp.where(lane < CHP, f1, jnp.where(lane < CHQ, f2, ZERO))

        def column(v, lane_at, n):
            c = jnp.sum(v, axis=I1, keepdims=True)
            c = jnp.concatenate([c, jnp.zeros((HIDP - n, I1), F32)], axis=I0)
            return jnp.where(lane == lane_at, c, ZERO)
        gn = gnbuf[k]
        mean = jnp.sum(gn, axis=I0, keepdims=True) * (ONE / 160.0) + EPS
        out = out + column(acc_beta[:, I0:LANE] + acc_beta[:, LANE:PXL], CHQ, HID)
        out = out + column((acc_cross[:, I0:LANE] + acc_cross[:, LANE:PXL]) * (gn / mean), 89, HID)
        for j in range(RAD):
            out = out + column(acc_n[j, :, I0:LANE] + acc_n[j, :, LANE:PXL], 90 + j, CH)
        gb[k, I0:HIDP, :] = out
        gb[k, HIDP:192, :] = jnp.zeros((PR, LANE), F32)

    def conv_backward(dy, out):
        def finish(g, hp, acc):
            v = acc.reshape(SUB, PR, PXL) + dy[g, pl.ds(SUB * hp, SUB)].astype(F32)
            out[g, pl.ds(SUB * hp, SUB)] = v.astype(BF16)
        conv(dp, finish)

    def scatter_copies(k):
        return [pltpu.make_async_remote_copy(
            src_ref=gb.at[k, pl.ds(pl.multiple_of(lax.rem(me + d, SUB) * NPAIR, SUB), NPAIR)], dst_ref=grx.at[k, d - I1],
            send_sem=gs_sem.at[k, d - I1], recv_sem=gr_sem.at[k, d - I1],
            device_id=peer(d), device_id_type=MESH) for d in range(I1, SUB)]

    def gather_copies(k):
        return [pltpu.make_async_remote_copy(
            src_ref=gs.at[k, TAP], dst_ref=gs.at[k, d - I1], send_sem=as2_sem.at[k, d - I1], recv_sem=ar2_sem.at[k, d - I1],
            device_id=peer(d), device_id_type=MESH) for d in range(I1, SUB)]

    def tap_copies(k):
        return [pltpu.make_async_remote_copy(
            src_ref=tx.at[k, me], dst_ref=tx.at[k, me], send_sem=ts_sem.at[k, d - I1], recv_sem=tr_sem.at[k, d - I1],
            device_id=peer(d), device_id_type=MESH) for d in range(I1, SUB)]

    def start_all(copies):
        for c in copies:
            c.start()

    def wait_all(copies):
        for c in copies:
            c.wait()

    def scatter_to_gather(k):
        wait_all(scatter_copies(k))
        mine = gb[k, pl.ds(pl.multiple_of(me * NPAIR, SUB), NPAIR), :]
        for d in range(TAP):
            mine = mine + grx[k, d]
        gs[k, TAP] = mine
        start_all(gather_copies(k))

    def to_x1(g, h, wp, v):
        x1[g, RAD + h, PAIR + wp] = v

    def to_gout(g, h, wp, v):
        gout[g, QUAD * h + wp] = v
    for c in range(QUAD):
        fetch(xin, c).start()
    for c in range(QUAD):
        fetch(xin, c).wait()
    load_tiles(to_x1)
    for c in range(QUAD):
        fetch(gin, c).start()
    pl.semaphore_wait(barrier, TAP)
    halo_start(x1, I0)
    setup()
    build_band(I0, I0)
    halo_local(x1)
    halo_finish(x1, I0)
    conv_forward(I0, x1)
    hidden_forward(I0, False)
    sa[I0, I0:CH] = pack_sums(fold(acc_g2))
    reduce_start(I0, CH)
    for c in range(QUAD):
        fetch(gin, c).wait()
    load_tiles(to_gout)
    build_band(I0, I1)
    total = reduce_finish(I0, CH)
    scale_from(I0, total)
    block1_out()
    halo_start(x2, I1)
    halo_local(x2)
    resp_phase(I1, gout, False)
    halo_finish(x2, I1)
    conv_forward(I1, x2)
    hidden_forward(I1, True)
    sa[I1, I0:CH] = pack_sums(fold(acc_g2))
    sa[I1, CH:80] = pack_sums(fold(acc_cross))
    reduce_start(I1, 80)
    build_band(I1, I1)
    slope_phase(I1)
    total = reduce_finish(I1, 80)
    scale_from(I1, total[I0:CH])
    grn_grad(I1, total[CH:80])
    hidden_backward(I1, gout, True)
    halo_start(dp, PAIR)
    halo_local(dp)
    conv_wgrad(I1, x2)
    store_grads(I1)
    halo_finish(dp, PAIR)
    start_all(scatter_copies(I1))
    start_all(tap_copies(I1))
    conv_backward(gout, dmid)
    resp_phase(I0, dmid, True)
    sa[PAIR, I0:CH] = pack_sums(fold(acc_cross))
    reduce_start(PAIR, CH)
    build_band(I1, I0)
    slope_phase(I0)
    unload_tiles(ytile, act_out)
    total = reduce_finish(PAIR, CH)
    grn_grad(I0, total)
    scatter_to_gather(I1)
    hidden_backward(I0, dmid, False)
    halo_start(dp, RAD)
    store_grads(I0)
    start_all(scatter_copies(I0))
    conv_wgrad(I0, x1)
    start_all(tap_copies(I0))
    halo_local(dp)
    scatter_to_gather(I0)
    halo_finish(dp, RAD)
    conv_backward(dmid, dmid)
    unload_wait(act_out)
    unload_tiles(dmid, grad_in)
    for k in range(PAIR):
        wait_all(tap_copies(k))
        wait_all(gather_copies(k))
        total = tx[k, I0]
        for d in range(I1, SUB):
            total = total + tx[k, d]
        tsum[k] = total
        grf[k, me] = gs[k, TAP]
        for d in range(I1, SUB):
            grf[k, lax.rem(me + SUB - d, SUB)] = gs[k, d - I1]
        gb[k] = grf[k].reshape(192, LANE)
    for k in range(PAIR):
        t = jnp.transpose(gb[k, I0:HID, :])
        o_w1[k] = t[I0:CH]
        o_w2[k] = t[CHP:CHQ] * KEEP
        o_b1[k:k + I1, :] = t[CH:41]
        o_beta[k:k + I1, :] = t[CHQ:89]
        o_gamma[k:k + I1, :] = t[89:90]
        o_gnorm[k:k + I1, :] = t[90:91, I0:CH]
        o_bnorm[k:k + I1, :] = t[91:92, I0:CH]
        o_bconv[k:k + I1, :] = t[92:93, I0:CH]
        o_b2[k:k + I1, :] = gb[k, HID:161, CHP:CHQ] * KEEP
    place = lax.broadcasted_iota(jnp.int32, (PAIR, LANE), I1) // SUB

    def taps_row(i, carry):
        for j in range(TAP):
            out = jnp.zeros((PAIR, LANE), F32)
            for g in range(NG):
                rows = jnp.concatenate([tsum[k, pl.ds(SUB * g + i, I1), :] for k in range(PAIR)], axis=I0)
                out = jnp.where(place == g, pltpu.roll(rows, (LANE + SUB * (g - j)) % LANE, I1), out)
            o_taps[i, j] = out[:, I0:CH]
        return carry
    lax.fori_loop(I0, TAP, taps_row, I0)
    unload_wait(grad_in)


def run_kernel(args):
    vm = pl.BlockSpec(memory_space=pltpu.VMEM)
    hbm = pl.BlockSpec(memory_space=pl.ANY)
    pad = pltpu.VMEM((NG, PADH, SUB, PR, PXL), BF16)
    tiles = pltpu.VMEM((NG, NPAIR, PR, PXL), BF16)
    return pl.pallas_call(
        kernel,
        name='blocks',
        out_shape=out_shapes(),
        in_specs=[hbm] * PAIR + [vm] * (len(args) - PAIR),
        out_specs=(hbm,) * PAIR + (vm,) * 10,
        scratch_shapes=[
            pltpu.VMEM((IMG, PADH, IMG, CH), BF16), pltpu.VMEM((2112, CH), F32), tiles, tiles,
            pltpu.VMEM((PAIR, SUB, PXL), F32), pltpu.VMEM((PAIR, NG, SUB, SUB, LANE), F32), pltpu.VMEM((PAIR, 640, LANE), F32),
            pltpu.VMEM((PAIR, HID, CHP), BF16), pltpu.VMEM((PAIR, HID, CH), BF16),
            pad, pad, pad,
            pltpu.VMEM((PAIR, NG, NPAIR, PR, PXL), BF16),
            pltpu.VMEM((PAIR, NPAIR, CHP, PXP), BF16),
            pltpu.VMEM((PAIR, NPAIR, HID, PXP), BF16),
            pltpu.VMEM((NPAIR, HID, PXP), F32), pltpu.VMEM((NPAIR, HID, PXP), F32),
            pltpu.VMEM((NPAIR, HID, PXP), BF16),
            pltpu.VMEM((NG, NPAIR, PR, PXL), BF16),
            pltpu.VMEM((NG, LANE, BAND), BF16),
            pltpu.VMEM((HID, PXL), F32), pltpu.VMEM((HID, PXL), F32), pltpu.VMEM((HID, PXL), F32),
            pltpu.VMEM((RAD, CH, PXL), F32),
            pltpu.VMEM((HID, TQ), F32), pltpu.VMEM((HIDP, TQ), F32),
            pltpu.VMEM((LANE, BAND), F32),
            pltpu.VMEM((PAIR, HID, LANE), F32), pltpu.VMEM((PAIR, HID, LANE), F32), pltpu.VMEM((HID, LANE), F32),
            pltpu.VMEM((QUAD, NG, RAD, QUAD, PR, LANE), BF16), pltpu.VMEM((QUAD, NG, RAD, QUAD, PR, LANE), BF16),
            pltpu.VMEM((QUAD, NG, 120, LANE), BF16), pltpu.VMEM((QUAD, RAD, 120, LANE), BF16),
            pltpu.VMEM((RAD, 80, LANE), F32), pltpu.VMEM((RAD, TAP, 80, LANE), F32),
            pltpu.VMEM((PAIR, 192, LANE), F32), pltpu.VMEM((PAIR, TAP, NPAIR, LANE), F32), pltpu.VMEM((PAIR, SUB, NPAIR, LANE), F32),
            pltpu.VMEM((PAIR, SUB, NPAIR, LANE), F32), pltpu.VMEM((PAIR, SUB, CH, LANE), F32), pltpu.VMEM((PAIR, CH, LANE), F32),
            pltpu.SemaphoreType.DMA((PADH,)),
            pltpu.SemaphoreType.DMA((QUAD, NG)), pltpu.SemaphoreType.DMA((QUAD, NG)),
            pltpu.SemaphoreType.DMA((RAD, TAP)), pltpu.SemaphoreType.DMA((RAD, TAP)),
        ] + [pltpu.SemaphoreType.DMA((PAIR, TAP))] * TILEH,
        compiler_params=pltpu.CompilerParams(collective_id=I0, has_side_effects=True, vmem_limit_bytes=67043328),
    )(*args)


def out_shapes():
    shape = lambda *d: jax.ShapeDtypeStruct(d, F32)
    act = jax.ShapeDtypeStruct((IMG, PADH, IMG, CH), BF16)
    small, wide = shape(PAIR, CH), shape(PAIR, HID)
    return (act, act, shape(TAP, TAP, PAIR, CH), small, small, small, shape(PAIR, CH, HID), wide, wide, wide, shape(PAIR, CH, HID), small)


def finish_kernel(*refs):
    n = len(refs) // RAD
    src, dst, mid = refs[I0:n], refs[n:PAIR * n], refs[PAIR * n:RAD * n]
    in_sem, out_sem = refs[RAD * n:]
    moves = []
    for a in range(n):
        cuts = [slice(QUAD * c, QUAD * c + QUAD) for c in range(SUB)] if a < PAIR else [slice(None)]
        for cut in cuts:
            moves.append((src[a].at[cut], mid[a].at[cut], dst[a].at[cut]))
    ins = [pltpu.make_async_copy(m[I0], m[I1], in_sem.at[c]) for c, m in enumerate(moves)]
    outs = [pltpu.make_async_copy(m[I1], m[PAIR], out_sem.at[c]) for c, m in enumerate(moves)]
    for c in ins:
        c.start()
    for c, o in zip(ins, outs):
        c.wait()
        o.start()
    for o in outs:
        o.wait()


def finish(parts):
    n = len(parts)
    hbm = pl.BlockSpec(memory_space=pl.ANY)
    return pl.pallas_call(
        finish_kernel, name='finish', out_shape=out_shapes(),
        in_specs=[hbm] * n, out_specs=(hbm,) * n,
        scratch_shapes=[pltpu.VMEM(o.shape, o.dtype) for o in out_shapes()] + [pltpu.SemaphoreType.DMA((n + 14,))] * PAIR,
        compiler_params=pltpu.CompilerParams(vmem_limit_bytes=67043328),
    )(*parts)


def solution(mesh):
    act_spec = P('dp', 'sh', 'sw', None)
    rep = P()

    def local_step(act_in, drop_mask, grad_out, conv_w, conv_b, norm_g, norm_b, fc1_w, fc1_b, grn_gamma, grn_beta, fc2_w, fc2_b):
        parts = run_kernel((act_in, grad_out, drop_mask.T, conv_w.transpose(I1, PAIR, I0, RAD), fc1_b, grn_gamma, grn_beta,
                            conv_b, norm_g, norm_b, fc2_b, fc1_w, fc2_w.transpose(I0, PAIR, I1)))
        act_out, grad_in, taps, *rest = finish(parts)
        rest[TAP] = rest[TAP].transpose(I0, PAIR, I1)
        return (act_out, grad_in, taps.transpose(PAIR, I0, I1, RAD), *rest)

    return jax.shard_map(local_step, mesh=mesh,
                         in_specs=(act_spec, P('dp', None), act_spec) + (rep,) * 10,
                         out_specs=(act_spec, act_spec) + (P('dp'),) * 10,
                         check_vma=False)
```
